128 devices in a mesh: gx: 8 (over x_lo, y), gy: 16 (over z, x_hi, core).
Axes of the slice: x: 4 (x_hi: 2, x_lo: 2; x = x_hi * 2 + x_lo), y: 4, z: 4, core: 2. Of those that a mesh axis runs over, the one named last changes fastest.
Arguments:
- expert_grad: bfloat16 [8, 512, 14336], P('gx', None, 'gy'), may hold values from -40000 to 40000
- attn_grad: bfloat16 [8, 2048, 4096], P('gx', None, 'gy'), may hold values from -40000 to 40000
- expert_master: float32 [4096, 14336], P(('gx', 'gy')), may hold values from -0.75 to 0.75
- expert_moment: float32 [4096, 14336], P(('gx', 'gy')), may hold values from -6 to 6
- expert_second: float32 [4096, 14336], P(('gx', 'gy')), may hold values from 0.1 to 4
- attn_master: float32 [2048, 4096], P(('gx', 'gy')), may hold values from -0.75 to 0.75
- attn_moment: float32 [2048, 4096], P(('gx', 'gy')), may hold values from -6 to 6
- attn_second: float32 [2048, 4096], P(('gx', 'gy')), may hold values from 0.1 to 4
Outputs:
- expert_master_new: float32 [4096, 14336], P(('gx', 'gy'))
- expert_moment_new: float32 [4096, 14336], P(('gx', 'gy'))
- expert_second_new: float32 [4096, 14336], P(('gx', 'gy'))
- attn_master_new: float32 [2048, 4096], P(('gx', 'gy'))
- attn_moment_new: float32 [2048, 4096], P(('gx', 'gy'))
- attn_second_new: float32 [2048, 4096], P(('gx', 'gy'))
- expert_weight: bfloat16 [8, 512, 14336], P('gx', None, 'gy')
- attn_weight: bfloat16 [2048, 4096], P(None, 'gy')
The draws below stay inside these ranges and needn't reach their ends.
All inputs are finite; a program needn't handle non-finite values.
Results may differ from the reference program's by a relative error of at most 0.001.
Values may be sent and summed in bfloat16 or wider, within the bound.
No kernel may reach another device: no remote copies, remote signals or barrier semaphores. Data moves between devices by JAX's collectives and lax.ppermute only.
A program may use at most 64 MiB of HBM per device.

```python
import math
import jax
import jax.numpy as jnp
from jax import lax

E = 8
FF = 14336
QW = 4096
EROWS = 512
AROWS = 2048
REPLICAS = 8
NUMEL = 67108864


def draw_expert_grad(key, part):
    keys = jax.random.split(key, 3)
    row_scale = jnp.exp(jax.random.uniform(keys[1], (E, EROWS, 1), jnp.float32) * jnp.log(10.0))
    col_scale = jnp.exp(jax.random.uniform(keys[2], (1, 1, FF), jnp.float32) * jnp.log(10.0))
    position = jnp.arange(E * EROWS, dtype=jnp.float32).reshape(E, EROWS, 1) / (E * EROWS - 1)
    ramp = 10.0 ** position
    base = jnp.clip(jax.random.normal(keys[0], (E, EROWS, FF), jnp.float32), -6.0, 6.0)
    return (base * row_scale * col_scale * ramp).astype(jnp.bfloat16)


def draw_attn_grad(key, part):
    keys = jax.random.split(key, 3)
    row_scale = jnp.exp(jax.random.uniform(keys[1], (1, AROWS, 1), jnp.float32) * jnp.log(10.0))
    col_scale = jnp.exp(jax.random.uniform(keys[2], (1, 1, QW), jnp.float32) * jnp.log(10.0))
    replica_ramp = (2.0 ** (jnp.arange(REPLICAS, dtype=jnp.float32) / (REPLICAS - 1)))[:, None, None]
    position = (jnp.arange(AROWS, dtype=jnp.float32) / (AROWS - 1))[None, :, None]
    ramp = replica_ramp * 10.0 ** position
    base = jnp.clip(jax.random.normal(keys[0], (REPLICAS, AROWS, QW), jnp.float32), -6.0, 6.0)
    return (base * row_scale * col_scale * ramp).astype(jnp.bfloat16)


def shard_levels(stream_key, shape, shards, least, high):
    def one(axis_at, blocks):
        heights = jax.random.uniform(jax.random.fold_in(jax.random.fold_in(stream_key, 6), axis_at), (blocks,), jnp.float32, least / len(shards), high / len(shards))
        return jnp.repeat(jnp.exp(heights), shape[axis_at] // blocks).reshape((-1,) + (1,) * (len(shape) - axis_at - 1))

    factor_of = one(*shards[0])
    for cut in shards[1:]:
        factor_of = factor_of * one(*cut)
    return factor_of


def noise(rng, shape, width, most, cuts=(), held_as=jnp.bfloat16):
    factor_of = shard_levels(rng, shape, cuts, -0.22, 0.18) if cuts else 1.0
    values = jax.random.normal(rng, shape, jnp.float32) * width * factor_of
    return jnp.minimum(jnp.maximum(values, -most), most).astype(held_as)


def setup_inputs(seed: int = 0) -> dict:
    key_list = jax.random.split(jax.random.key(seed), 9)
    expert_grad = draw_expert_grad(jax.random.fold_in(key_list[8], 71), 0)
    attn_grad = draw_attn_grad(jax.random.fold_in(key_list[8], 71), 0)
    expert_master = noise(key_list[2], (E * EROWS, FF), 0.05, 0.75, ((0, 128),), jnp.float32)
    expert_moment = noise(key_list[3], (E * EROWS, FF), 1.0, 6.0, ((0, 128),), jnp.float32)
    expert_second = jnp.clip(jnp.exp(math.log(4.0) - 3.6888794 * jax.random.uniform(key_list[4], (E * EROWS, FF), jnp.float32) ** shard_levels(key_list[4], (E * EROWS, FF), ((0, 128),), -0.2, 0.2)), 0.1, 4.0)
    attn_master = noise(key_list[5], (AROWS, QW), 0.05, 0.75, ((0, 128),), jnp.float32)
    attn_moment = noise(key_list[6], (AROWS, QW), 1.0, 6.0, ((0, 128),), jnp.float32)
    attn_second = jnp.clip(jnp.exp(math.log(4.0) - 3.6888794 * jax.random.uniform(key_list[7], (AROWS, QW), jnp.float32) ** shard_levels(key_list[7], (AROWS, QW), ((0, 128),), -0.2, 0.2)), 0.1, 4.0)
    return {"expert_grad": expert_grad, "attn_grad": attn_grad, "expert_master": expert_master, "expert_moment": expert_moment, "expert_second": expert_second, "attn_master": attn_master, "attn_moment": attn_moment, "attn_second": attn_second}


beta_one = 0.9
beta_two = 0.95
learn_rate = 0.01
weight_decay = 0.1
adam_eps = 1e-08
bias_one = 1.0 - 0.9 ** 20
bias_two = 1.0 - 0.95 ** 20

def adam_update(gradient, master, moment, second, clip_factor):
    scaled = clip_factor * gradient
    moment_new = beta_one * moment + (1.0 - beta_one) * scaled
    second_new = beta_two * second + (1.0 - beta_two) * scaled * scaled
    update = moment_new / bias_one / (jnp.sqrt(second_new / bias_two) + adam_eps)
    master_new = master - learn_rate * (update + weight_decay * master)
    return (master_new, moment_new, second_new)

def reference(expert_grad, attn_grad, expert_master, expert_moment, expert_second, attn_master, attn_moment, attn_second):
    expert_flat = expert_grad.astype(jnp.float32).reshape(E * EROWS, FF)
    attn_sum = lax.optimization_barrier(jnp.sum(attn_grad.astype(jnp.float32), axis=0))
    total = jnp.sum(expert_flat * expert_flat) + jnp.sum(attn_sum * attn_sum)
    clip_factor = 1.0 / jnp.sqrt(total / NUMEL + 1e-06)
    e_master, e_moment, e_second = adam_update(expert_flat, expert_master, expert_moment, expert_second, clip_factor)
    a_master, a_moment, a_second = adam_update(attn_sum, attn_master, attn_moment, attn_second, clip_factor)
    expert_weight = e_master.astype(jnp.bfloat16).reshape(E, EROWS, FF)
    attn_weight = a_master.astype(jnp.bfloat16)
    return (e_master, e_moment, e_second, a_master, a_moment, a_second, expert_weight, attn_weight)
```

```python
import jax
import jax.numpy as jnp
from jax import lax
from jax.sharding import Mesh
from jax.sharding import PartitionSpec as P

NUMEL = 67108864
GY = ("gy_0", "gy_1", "gy_2")
GX = ("gx_0", "gx_1")
GX_GY = ("gx_0", "gx_1", "gy_0", "gy_1", "gy_2")


beta_one = 0.9
beta_two = 0.95
learn_rate = 0.01
weight_decay = 0.1
adam_eps = 1e-08
bias_one = 1.0 - 0.9**20
bias_two = 1.0 - 0.95**20


def cut_along(shard, dim, devices):
    before, after = (shard.shape[:dim], shard.shape[dim + 1 :])
    return jnp.moveaxis(shard.reshape(*before, devices, -1, *after), dim, 0)


def sum_at_owner(shard, axis, dim):
    parts = cut_along(shard, dim, lax.axis_size(axis))
    arrived = lax.all_to_all(parts, axis, split_axis=0, concat_axis=0, tiled=True)
    return arrived.astype(jnp.float32).sum(axis=0)


def sum_over_all(part, axes):
    copies = jnp.broadcast_to(part, (lax.axis_size(axes), 1, 128))
    arrived = lax.all_to_all(copies, axes, split_axis=0, concat_axis=0, tiled=True)
    return jnp.sum(arrived, axis=(0, 1))[0]


def joined_along(parts, dim):
    parts = jnp.moveaxis(parts, 0, dim)
    dims = parts.shape
    return parts.reshape(*dims[:dim], dims[dim] * dims[dim + 1], *dims[dim + 2 :])


def from_everyone(shard, axis):
    copies = jnp.broadcast_to(shard, (lax.axis_size(axis), *shard.shape))
    return lax.all_to_all(copies, axis, split_axis=0, concat_axis=0, tiled=True)


def gather_directly(shard, axis, dim):
    return joined_along(from_everyone(shard, axis), dim)


def adam_update(gradient, master, moment, second, clip_factor):
    scaled = clip_factor * gradient
    moment_new = beta_one * moment + (1.0 - beta_one) * scaled
    second_new = beta_two * second + (1.0 - beta_two) * scaled * scaled
    update = moment_new / bias_one / (jnp.sqrt(second_new / bias_two) + adam_eps)
    master_new = master - learn_rate * (update + weight_decay * master)
    return (master_new, moment_new, second_new)


def squares(expert_part, attn_part):
    wide = expert_part.astype(jnp.float32)
    return jnp.sum(wide * wide) + jnp.sum(attn_part * attn_part)


def regroup(flat_grad, owned):
    expert_group = lax.all_to_all(flat_grad, GY, split_axis=0, concat_axis=1, tiled=True)
    attn_group = lax.all_to_all(owned, GY, split_axis=0, concat_axis=1, tiled=True)
    return (expert_group, attn_group)


def local(
    expert_grad,
    attn_grad,
    expert_master,
    expert_moment,
    expert_second,
    attn_master,
    attn_moment,
    attn_second,
):
    local_experts, expert_rows, col_share = expert_grad.shape
    flat_grad = expert_grad.reshape(local_experts * expert_rows, col_share)
    attn_local = attn_grad.reshape(attn_grad.shape[1], attn_grad.shape[2])
    owned = sum_at_owner(attn_local, GX, 0)
    expert_group, attn_group = regroup(flat_grad, owned)
    total = sum_over_all(squares(flat_grad, owned), GX_GY)
    clip_factor = 1.0 / jnp.sqrt(total / NUMEL + 1e-06)
    e_master, e_moment, e_second = adam_update(
        expert_group.astype(jnp.float32), expert_master, expert_moment, expert_second, clip_factor
    )
    a_master, a_moment, a_second = adam_update(
        attn_group, attn_master, attn_moment, attn_second, clip_factor
    )
    expert_back, attn_back = (
        lax.all_to_all(e_master.astype(jnp.bfloat16), GY, split_axis=1, concat_axis=0, tiled=True),
        lax.all_to_all(a_master.astype(jnp.bfloat16), GY, split_axis=1, concat_axis=0, tiled=True),
    )
    expert_weight = expert_back.reshape(local_experts, expert_rows, col_share)
    attn_weight = gather_directly(attn_back, GX, 0)
    return (e_master, e_moment, e_second, a_master, a_moment, a_second, expert_weight, attn_weight)


def solution(mesh):
    split = Mesh(mesh.devices.reshape(2, 4, 4, 2, 2), ("gx_0", "gx_1", "gy_0", "gy_1", "gy_2"))
    placed = (
        P(GX, None, GY),
        P(GX, None, GY),
        P(GX_GY, None),
        P(GX_GY, None),
        P(GX_GY, None),
        P(GX_GY, None),
        P(GX_GY, None),
        P(GX_GY, None),
    )
    return jax.shard_map(
        local,
        mesh=split,
        in_specs=placed,
        out_specs=(
            P(GX_GY, None),
            P(GX_GY, None),
            P(GX_GY, None),
            P(GX_GY, None),
            P(GX_GY, None),
            P(GX_GY, None),
            P(GX, None, GY),
            P(None, GY),
        ),
        check_vma=False,
    )
```

```python
import jax
import jax.numpy as jnp
from jax import lax
from jax.experimental import pallas as pl
from jax.experimental.pallas import tpu as pltpu
from jax.sharding import Mesh
from jax.sharding import PartitionSpec as P


NUMEL = 67108864
GY = ("gy_0", "gy_1", "gy_2")
GX = ("gx_0", "gx_1")
GX_GY = ("gx_0", "gx_1", "gy_0", "gy_1", "gy_2")
bf16 = jnp.bfloat16
f32 = jnp.float32

beta_one = 0.9
beta_two = 0.95
learn_rate = 0.01
weight_decay = 0.1
adam_eps = 1e-08
bias_one = 1.0 - 0.9**20
bias_two = 1.0 - 0.95**20

ROWS, COLS = 32, 896
AROWS, ACOLS = 16, 256
STATE = 3 * ACOLS
WIDE = COLS + STATE
BACK = COLS + ACOLS

CHIP_STEPS = ((1, 0), (3, 0), (2, 0), (0, 1), (1, 1), (3, 1), (2, 1))
REPLICA_STEPS = ((0, 1), (0, 3), (0, 2), (1, 0), (1, 1), (1, 3), (1, 2))


def call(kernel, out, flops, mib=12, **kw):
    return pl.pallas_call(
        kernel,
        out_shape=out,
        cost_estimate=pl.CostEstimate(flops=flops, bytes_accessed=4096, transcendentals=0),
        compiler_params=pltpu.CompilerParams(vmem_limit_bytes=mib * 2**20),
        **kw,
    )


def shape(dims, dtype):
    return jax.ShapeDtypeStruct(dims, dtype)


def halves(x):
    high = x.astype(bf16)
    return high, (x - high.astype(f32)).astype(bf16)


def adam_update(gradient, master, moment, second, clip_factor):
    scaled = clip_factor * gradient
    moment_new = beta_one * moment + (1.0 - beta_one) * scaled
    second_new = beta_two * second + (1.0 - beta_two) * scaled * scaled
    update = moment_new / bias_one / (jnp.sqrt(second_new / bias_two) + adam_eps)
    master_new = master - learn_rate * (update + weight_decay * master)
    return (master_new, moment_new, second_new)


def clip_of(sums_ref):
    total = jnp.sum(jnp.sum(sums_ref[...], axis=0, keepdims=True), axis=1, keepdims=True)
    return 1.0 / jnp.sqrt(total / NUMEL + 1e-06)


def fold_lanes(x):
    total = x[:, :128]
    for at in range(128, x.shape[1], 128):
        total = total + x[:, at : at + 128]
    return jnp.sum(total, axis=0, keepdims=True)


def pack_kernel(grad, master, moment, second, own, swap, part):
    core = lax.axis_index("gy_2")
    total = jnp.zeros((8, COLS), f32)
    for chip in range(8):
        for out, which in ((own, core), (swap, 1 - core)):
            rows = grad[2 * chip + which]
            out[chip, :, :COLS] = rows
            wide = rows.astype(f32)
            total = total + jnp.sum((wide * wide).reshape(ROWS // 8, 8, COLS), axis=0)
            cols = pl.ds(pl.multiple_of((2 * chip + which) * ACOLS, ACOLS), ACOLS)
            for n, state in enumerate((master, moment, second)):
                high, low = halves(state[:, cols])
                at = COLS + n * ACOLS
                out[chip, :AROWS, at : at + ACOLS] = high
                out[chip, AROWS:, at : at + ACOLS] = low
    part[...] = fold_lanes(total)


def route_kernel(own, swapped, *outs):
    z, x, core = (lax.axis_index(axis) for axis in GY)
    for (dz, dx), out in zip(((0, 0),) + CHIP_STEPS, outs):
        chip = lax.rem(z + dz, 4) * 2 + lax.rem(x + dx, 2)
        out[core] = own[chip]
        out[1 - core] = swapped[chip]


def sum_kernel(arrived, part, summed, partial):
    total = arrived[0].astype(f32)
    for replica in range(1, 8):
        total = total + arrived[replica].astype(f32)
    summed[...] = total
    squared = jnp.sum((total * total).reshape(32, 8, ACOLS), axis=0)
    partial[...] = part[...] + fold_lanes(squared)


def expert_weight_kernel(where, sums, grad, master, moment, second, attn, out):
    clip = clip_of(sums)
    for core in range(2):
        cols = slice(core * COLS, (core + 1) * COLS)
        new, _, _ = adam_update(
            grad[0, core].astype(f32), master[:, cols], moment[:, cols], second[:, cols], clip
        )
        out[core, :, :COLS] = new.astype(bf16)
        high, low = halves(attn[core * AROWS : (core + 1) * AROWS, :])
        out[core, :AROWS, COLS:] = high
        out[core, AROWS:, COLS:] = low


def expert_state_kernel(where, sums, grad, master, moment, second, master_new, moment_new, second_new):
    clip = clip_of(sums)
    for core in range(2):
        cols = slice(core * COLS, (core + 1) * COLS)
        master_new[:, cols], moment_new[:, cols], second_new[:, cols] = adam_update(
            grad[0, core].astype(f32), master[:, cols], moment[:, cols], second[:, cols], clip
        )


def attn_weight_kernel(sums, attn, *refs):
    arrived, out = refs[:-1], refs[-1]
    z, x = (lax.axis_index(axis) for axis in GY[:2])
    clip = clip_of(sums)
    for (dz, dx), block in zip(((0, 0),) + CHIP_STEPS, arrived):
        chip = lax.rem(z + 4 - dz, 4) * 2 + lax.rem(x + dx, 2)
        for core in range(2):
            rows = pl.ds(pl.multiple_of((chip * 2 + core) * AROWS, AROWS), AROWS)
            high = block[core, :AROWS, COLS:].astype(f32)
            low = block[core, AROWS:, COLS:].astype(f32)
            state = high + low
            new, _, _ = adam_update(
                attn[rows, :],
                state[:, :ACOLS],
                state[:, ACOLS : 2 * ACOLS],
                state[:, 2 * ACOLS :],
                clip,
            )
            out[rows, :] = new.astype(bf16)


def join_kernel(*refs):
    pieces, out = refs[:-1], refs[-1]
    x, y = (lax.axis_index(axis) for axis in GX)
    for (dx, dy), piece in zip(((0, 0),) + REPLICA_STEPS, pieces):
        out[lax.rem(x + dx, 2) * 4 + lax.rem(y + 4 - dy, 4)] = piece[...]


def finish_kernel(sums, arrived, master, moment, second, weight, master_new, moment_new, second_new):
    clip = clip_of(sums)
    for group in range(16):
        weight[group] = arrived[group, :, :COLS]
        cols = slice(group * ACOLS, (group + 1) * ACOLS)
        gradient = arrived[group, :AROWS, COLS:].astype(f32) + arrived[group, AROWS:, COLS:].astype(f32)
        master_new[:, cols], moment_new[:, cols], second_new[:, cols] = adam_update(
            gradient, master[:, cols], moment[:, cols], second[:, cols], clip
        )


def chip_pairs(dz, dx):
    return [(z * 2 + x, (z + dz) % 4 * 2 + (x + dx) % 2) for z in range(4) for x in range(2)]


def replica_pairs(dx, dy):
    return [(x * 4 + y, (x + dx) % 2 * 4 + (y + dy) % 4) for x in range(2) for y in range(4)]


def local(
    expert_grad,
    attn_grad,
    expert_master,
    expert_moment,
    expert_second,
    attn_master,
    attn_moment,
    attn_second,
):
    arrived = lax.all_to_all(
        attn_grad.reshape(8, 256, ACOLS), GX, split_axis=0, concat_axis=0, tiled=True
    )

    own, swap, part = call(
        pack_kernel,
        (shape((8, ROWS, WIDE), bf16), shape((8, ROWS, WIDE), bf16), shape((1, 128), f32)),
        4000000,
    )(expert_grad.reshape(16, ROWS, COLS), attn_master, attn_moment, attn_second)
    swapped = lax.ppermute(swap, "gy_2", [(0, 1), (1, 0)])
    routed = call(route_kernel, (shape((2, ROWS, WIDE), bf16),) * 8, 1000000)(own, swapped)
    blocks = [routed[0]]
    for n, step in enumerate(CHIP_STEPS):
        blocks.append(lax.ppermute(routed[n + 1], GY[:2], chip_pairs(*step)))

    attn_sum, partial = call(
        sum_kernel, (shape((256, ACOLS), f32), shape((1, 128), f32)), 2000000
    )(arrived, part)
    sums = lax.all_to_all(
        jnp.broadcast_to(partial, (128, 1, 128)), GX_GY, split_axis=0, concat_axis=0, tiled=True
    ).reshape(128, 128)

    order = {step: n for n, step in enumerate(((0, 0),) + CHIP_STEPS)}
    grads = jnp.stack([blocks[order[(n // 2, n % 2)]][:, :, :COLS] for n in range(8)])
    where = jnp.stack([lax.axis_index("gy_0"), lax.axis_index("gy_1")]).astype(jnp.int32)

    def source(n, at):
        return (lax.rem(at[0] + 4 - n // 2, 4) * 2 + lax.rem(at[1] + n, 2), 0, 0, 0)

    rows = pl.BlockSpec((ROWS, 2 * COLS), lambda n, at: (0, n))
    inputs = [
        pl.BlockSpec((128, 128), lambda n, at: (0, 0)),
        pl.BlockSpec((1, 2, ROWS, COLS), source),
        rows,
        rows,
        rows,
    ]
    state = (expert_master, expert_moment, expert_second)
    weights = call(
        expert_weight_kernel,
        shape((16, ROWS, BACK), bf16),
        4000000,
        grid_spec=pltpu.PrefetchScalarGridSpec(
            num_scalar_prefetch=1,
            grid=(8,),
            in_specs=inputs + [pl.BlockSpec((2 * AROWS, ACOLS), lambda n, at: (n, 0))],
            out_specs=pl.BlockSpec((2, ROWS, BACK), lambda n, at: (n, 0, 0)),
        ),
    )(where, sums, grads, *state, attn_sum)
    returned = lax.all_to_all(weights, GY, split_axis=0, concat_axis=0, tiled=True)
    attn_block = call(attn_weight_kernel, shape((256, ACOLS), bf16), 2000000)(
        sums, attn_sum, *blocks
    )
    pieces = [attn_block]
    for step in REPLICA_STEPS:
        pieces.append(lax.ppermute(attn_block, GX, replica_pairs(*step)))
    e_master, e_moment, e_second = call(
        expert_state_kernel,
        (shape((ROWS, 16 * COLS), f32),) * 3,
        8000000,
        grid_spec=pltpu.PrefetchScalarGridSpec(
            num_scalar_prefetch=1, grid=(8,), in_specs=inputs, out_specs=[rows] * 3
        ),
    )(where, sums, grads, *state)
    attn_weight = call(join_kernel, shape((8, 256, ACOLS), bf16), 1000000)(*pieces)
    expert_weight, a_master, a_moment, a_second = call(
        finish_kernel,
        (shape((16, ROWS, COLS), bf16),) + (shape((AROWS, 16 * ACOLS), f32),) * 3,
        2000000,
    )(sums, returned, attn_master, attn_moment, attn_second)
    return (
        e_master,
        e_moment,
        e_second,
        a_master,
        a_moment,
        a_second,
        expert_weight.reshape(1, 16 * ROWS, COLS),
        attn_weight.reshape(2048, ACOLS),
    )


def solution(mesh):
    split = Mesh(mesh.devices.reshape(2, 4, 4, 2, 2), GX_GY)
    placed = (P(GX, None, GY),) * 2 + (P(GX_GY, None),) * 6

    return jax.shard_map(
        local,
        mesh=split,
        in_specs=placed,
        out_specs=(P(GX_GY, None),) * 6 + (P(GX, None, GY), P(None, GY)),
        check_vma=False,
    )
```

```python
import jax
import jax.numpy as jnp
from jax import lax
from jax.experimental import pallas as pl
from jax.experimental.pallas import tpu as pltpu
from jax.sharding import Mesh
from jax.sharding import PartitionSpec as P


NUMEL = 67108864
GY = ("gy_0", "gy_1", "gy_2")
GX = ("gx_0", "gx_1")
GX_GY = ("gx_0", "gx_1", "gy_0", "gy_1", "gy_2")
bf16 = jnp.bfloat16
f32 = jnp.float32

beta_one = 0.9
beta_two = 0.95
learn_rate = 0.01
weight_decay = 0.1
adam_eps = 1e-08
bias_one = 1.0 - 0.9**20
bias_two = 1.0 - 0.95**20

ROWS, COLS = 32, 896
AROWS, ACOLS = 16, 256
STATE = 3 * ACOLS
WIDE = COLS + STATE
BACK = COLS + ACOLS

CHIP_STEPS = ((1, 0), (3, 0), (2, 0), (0, 1), (1, 1), (3, 1), (2, 1))
REPLICA_STEPS = (1, 3, 2)


def call(kernel, out, flops, mib=12, **kw):
    return pl.pallas_call(
        kernel,
        out_shape=out,
        cost_estimate=pl.CostEstimate(flops=flops, bytes_accessed=4096, transcendentals=0),
        compiler_params=pltpu.CompilerParams(vmem_limit_bytes=mib * 2**20),
        **kw,
    )


def shape(dims, dtype):
    return jax.ShapeDtypeStruct(dims, dtype)


def halves(x):
    high = x.astype(bf16)
    return high, (x - high.astype(f32)).astype(bf16)


def adam_update(gradient, master, moment, second, clip_factor):
    scaled = clip_factor * gradient
    moment_new = beta_one * moment + (1.0 - beta_one) * scaled
    second_new = beta_two * second + (1.0 - beta_two) * scaled * scaled
    mean_square = second_new * (1.0 / bias_two)
    root = mean_square * lax.rsqrt(mean_square)
    update = moment_new * (1.0 / bias_one) / (root + adam_eps)
    master_new = master - learn_rate * (update + weight_decay * master)
    return (master_new, moment_new, second_new)


def clip_of(sums_ref):
    total = jnp.sum(jnp.sum(sums_ref[...], axis=0, keepdims=True), axis=1, keepdims=True)
    return 1.0 / jnp.sqrt(total / NUMEL + 1e-06)


def fold_lanes(x):
    total = x[:, :128]
    for at in range(128, x.shape[1], 128):
        total = total + x[:, at : at + 128]
    return jnp.sum(total, axis=0, keepdims=True)


def pack_kernel(grad, master, moment, second, own, swap, part):
    core = lax.axis_index("gy_2")
    total = jnp.zeros((8, COLS), f32)
    for chip in range(8):
        for out, which in ((own, core), (swap, 1 - core)):
            rows = grad[2 * chip + which]
            out[chip, :, :COLS] = rows
            wide = rows.astype(f32)
            total = total + jnp.sum((wide * wide).reshape(ROWS // 8, 8, COLS), axis=0)
            cols = pl.ds(pl.multiple_of((2 * chip + which) * ACOLS, ACOLS), ACOLS)
            for n, state in enumerate((master, moment, second)):
                high, low = halves(state[:, cols])
                at = COLS + n * ACOLS
                out[chip, :AROWS, at : at + ACOLS] = high
                out[chip, AROWS:, at : at + ACOLS] = low
    part[...] = fold_lanes(total)


def route_kernel(own, swapped, *outs):
    z, x, core = (lax.axis_index(axis) for axis in GY)
    for (dz, dx), out in zip(((0, 0),) + CHIP_STEPS, outs):
        chip = lax.rem(z + dz, 4) * 2 + lax.rem(x + dx, 2)
        out[core] = own[chip]
        out[1 - core] = swapped[chip]


def sum_kernel(arrived, part, summed, copies):
    total = arrived[0].astype(f32)
    for replica in range(1, 8):
        total = total + arrived[replica].astype(f32)
    summed[...] = total
    squared = jnp.sum((total * total).reshape(32, 8, ACOLS), axis=0)
    copies[...] = jnp.broadcast_to(part[...] + fold_lanes(squared), (128, 128))


def sources():
    z, x = (lax.axis_index(axis) for axis in GY[:2])
    return [
        lax.rem(z + 4 - dz, 4) * 2 + lax.rem(x + dx, 2) for dz, dx in ((0, 0),) + CHIP_STEPS
    ]


def wide_cols(chip):
    return pl.ds(pl.multiple_of(chip * 2 * COLS, 2 * COLS), 2 * COLS)


def lanes(at):
    return slice(at * 128, (at + 1) * 128)


def expert_loads(blocks, state, held, grads, sems):
    loads = []
    for n, (chip, block) in enumerate(zip(sources(), blocks)):
        copies = [pltpu.make_async_copy(block.at[:, :, :COLS], grads.at[n], sems.at[n, 3])]
        for m, array in enumerate(state):
            copies.append(
                pltpu.make_async_copy(array.at[:, wide_cols(chip)], held.at[m, n], sems.at[n, m])
            )
        for copy in copies:
            copy.start()
        loads.append(copies)
    return loads


def expert_weight_kernel(sums, attn, *refs):
    blocks, state, out = refs[:8], refs[8:11], refs[11]
    held, grads, weights, sems, out_sems = refs[12:]
    loads = expert_loads(blocks, state, held, grads, sems)
    clip = clip_of(sums)
    stores = []
    for n, chip in enumerate(sources()):
        for core in range(2):
            rows = pl.ds(pl.multiple_of((chip * 2 + core) * AROWS, AROWS), AROWS)
            high, low = halves(attn[rows, :])
            weights[n, core, :AROWS, COLS:] = high
            weights[n, core, AROWS:, COLS:] = low
        for copy in loads[n]:
            copy.wait()
        for at in range(14):
            core, col = divmod(at, 7)
            new, _, _ = adam_update(
                grads[n, core, :, lanes(col)].astype(f32),
                held[0, n, :, lanes(at)],
                held[1, n, :, lanes(at)],
                held[2, n, :, lanes(at)],
                clip,
            )
            weights[n, core, :, lanes(col)] = new.astype(bf16)
        store = pltpu.make_async_copy(weights.at[n], out.at[pl.ds(chip * 2, 2)], out_sems.at[n])
        store.start()
        stores.append(store)
    for store in stores:
        store.wait()


def expert_state_kernel(sums, *refs):
    blocks, state, outs = refs[:8], refs[8:11], refs[11:14]
    held, grads, news, sems, out_sems = refs[14:]
    loads = expert_loads(blocks, state, held, grads, sems)
    clip = clip_of(sums)
    stores = []
    for n, chip in enumerate(sources()):
        for copy in loads[n]:
            copy.wait()
        for at in range(14):
            core, col = divmod(at, 7)
            results = adam_update(
                grads[n, core, :, lanes(col)].astype(f32),
                held[0, n, :, lanes(at)],
                held[1, n, :, lanes(at)],
                held[2, n, :, lanes(at)],
                clip,
            )
            for m, result in enumerate(results):
                news[m, n, :, lanes(at)] = result
        for m, out in enumerate(outs):
            store = pltpu.make_async_copy(
                news.at[m, n], out.at[:, wide_cols(chip)], out_sems.at[n, m]
            )
            store.start()
            stores.append(store)
    for store in stores:
        store.wait()


def attn_weight_kernel(sums, attn, *refs):
    blocks, out, held, sems = refs[:8], refs[8], refs[9], refs[10]
    loads = []
    for n, block in enumerate(blocks):
        copy = pltpu.make_async_copy(block.at[:, :, COLS:], held.at[n], sems.at[n])
        copy.start()
        loads.append(copy)
    clip = clip_of(sums)
    for n, chip in enumerate(sources()):
        loads[n].wait()
        for core in range(2):
            rows = pl.ds(pl.multiple_of((chip * 2 + core) * AROWS, AROWS), AROWS)
            state = held[n, core, :AROWS, :].astype(f32) + held[n, core, AROWS:, :].astype(f32)
            new, _, _ = adam_update(
                attn[rows, :],
                state[:, :ACOLS],
                state[:, ACOLS : 2 * ACOLS],
                state[:, 2 * ACOLS :],
                clip,
            )
            out[rows, :] = new.astype(bf16)


def both_kernel(own, other, out):
    x = lax.axis_index("gx_0")
    out[x] = own[...]
    out[1 - x] = other[...]


def join_kernel(*refs):
    pieces, out = refs[:-1], refs[-1]
    y = lax.axis_index("gx_1")
    for dy, piece in zip((0,) + REPLICA_STEPS, pieces):
        for x in range(2):
            out[x * 4 + lax.rem(y + 4 - dy, 4)] = piece[x]


def finish_kernel(sums, arrived, master, moment, second, weight, master_new, moment_new, second_new):
    clip = clip_of(sums)
    for group in range(16):
        weight[group] = arrived[group, :, :COLS]
        cols = slice(group * ACOLS, (group + 1) * ACOLS)
        gradient = arrived[group, :AROWS, COLS:].astype(f32) + arrived[group, AROWS:, COLS:].astype(f32)
        master_new[:, cols], moment_new[:, cols], second_new[:, cols] = adam_update(
            gradient, master[:, cols], moment[:, cols], second[:, cols], clip
        )


def chip_pairs(dz, dx):
    return [(z * 2 + x, (z + dz) % 4 * 2 + (x + dx) % 2) for z in range(4) for x in range(2)]


def local(
    expert_grad,
    attn_grad,
    expert_master,
    expert_moment,
    expert_second,
    attn_master,
    attn_moment,
    attn_second,
):
    arrived = lax.all_to_all(
        attn_grad.reshape(8, 256, ACOLS), GX, split_axis=0, concat_axis=0, tiled=True
    )

    own, swap, part = call(
        pack_kernel,
        (shape((8, ROWS, WIDE), bf16), shape((8, ROWS, WIDE), bf16), shape((1, 128), f32)),
        4000000,
    )(expert_grad.reshape(16, ROWS, COLS), attn_master, attn_moment, attn_second)
    swapped = lax.ppermute(swap, "gy_2", [(0, 1), (1, 0)])
    routed = call(route_kernel, (shape((2, ROWS, WIDE), bf16),) * 8, 1000000)(own, swapped)
    blocks = [routed[0]]
    for n, step in enumerate(CHIP_STEPS):
        blocks.append(lax.ppermute(routed[n + 1], GY[:2], chip_pairs(*step)))

    attn_sum, partial = call(
        sum_kernel, (shape((256, ACOLS), f32), shape((128, 128), f32)), 2000000
    )(arrived, part)
    sums = lax.all_to_all(
        partial.reshape(128, 1, 128), GX_GY, split_axis=0, concat_axis=0, tiled=True
    ).reshape(128, 128)

    here = pl.BlockSpec(memory_space=pltpu.VMEM)
    far = pl.BlockSpec(memory_space=pltpu.HBM)
    state = (expert_master, expert_moment, expert_second)
    attn_block = call(
        attn_weight_kernel,
        shape((256, ACOLS), bf16),
        2000000,
        in_specs=[here] * 2 + [far] * 8,
        out_specs=here,
        scratch_shapes=[
            pltpu.VMEM((8, 2, ROWS, STATE), bf16),
            pltpu.SemaphoreType.DMA((8,)),
        ],
    )(sums, attn_sum, *blocks)
    other = lax.ppermute(attn_block, "gx_0", [(0, 1), (1, 0)])
    weights = call(
        expert_weight_kernel,
        shape((16, ROWS, BACK), bf16),
        8000000,
        mib=63,
        in_specs=[here] * 2 + [far] * 11,
        out_specs=far,
        scratch_shapes=[
            pltpu.VMEM((3, 8, ROWS, 2 * COLS), f32),
            pltpu.VMEM((8, 2, ROWS, COLS), bf16),
            pltpu.VMEM((8, 2, ROWS, BACK), bf16),
            pltpu.SemaphoreType.DMA((8, 4)),
            pltpu.SemaphoreType.DMA((8,)),
        ],
    )(sums, attn_sum, *blocks, *state)
    returned = lax.all_to_all(weights, GY, split_axis=0, concat_axis=0, tiled=True)
    both = call(both_kernel, shape((2, 256, ACOLS), bf16), 1000000)(attn_block, other)
    pieces = [both]
    for n in range(3):
        pieces.append(
            lax.ppermute(both, "gx_1", [(y, (y + REPLICA_STEPS[n]) % 4) for y in range(4)])
        )
    e_master, e_moment, e_second = call(
        expert_state_kernel,
        (shape((ROWS, 16 * COLS), f32),) * 3,
        8000000,
        mib=63,
        in_specs=[here] + [far] * 11,
        out_specs=[far] * 3,
        scratch_shapes=[
            pltpu.VMEM((3, 8, ROWS, 2 * COLS), f32),
            pltpu.VMEM((8, 2, ROWS, COLS), bf16),
            pltpu.VMEM((3, 8, ROWS, 2 * COLS), f32),
            pltpu.SemaphoreType.DMA((8, 4)),
            pltpu.SemaphoreType.DMA((8, 3)),
        ],
    )(sums, *blocks, *state)
    attn_weight = call(join_kernel, shape((8, 256, ACOLS), bf16), 1000000)(*pieces)
    expert_weight, a_master, a_moment, a_second = call(
        finish_kernel,
        (shape((16, ROWS, COLS), bf16),) + (shape((AROWS, 16 * ACOLS), f32),) * 3,
        2000000,
    )(sums, returned, attn_master, attn_moment, attn_second)
    return (
        e_master,
        e_moment,
        e_second,
        a_master,
        a_moment,
        a_second,
        expert_weight.reshape(1, 16 * ROWS, COLS),
        attn_weight.reshape(2048, ACOLS),
    )


def solution(mesh):
    split = Mesh(mesh.devices.reshape(2, 4, 4, 2, 2), GX_GY)
    placed = (P(GX, None, GY),) * 2 + (P(GX_GY, None),) * 6

    return jax.shard_map(
        local,
        mesh=split,
        in_specs=placed,
        out_specs=(P(GX_GY, None),) * 6 + (P(GX, None, GY), P(None, GY)),
        check_vma=False,
    )
```

```python
import jax
import jax.numpy as jnp
from jax import lax
from jax.experimental import pallas as pl
from jax.experimental.pallas import tpu as pltpu
from jax.sharding import Mesh
from jax.sharding import PartitionSpec as P


NUMEL = 67108864
GY = ("gy_0", "gy_1", "gy_2")
GX = ("gx_0", "gx_1")
GX_GY = ("gx_0", "gx_1", "gy_0", "gy_1", "gy_2")
bf16 = jnp.bfloat16
f32 = jnp.float32

beta_one = 0.9
beta_two = 0.95
learn_rate = 0.01
weight_decay = 0.1
adam_eps = 1e-08
bias_one = 1.0 - 0.9**20
bias_two = 1.0 - 0.95**20

ROWS, COLS = 32, 896
AROWS, ACOLS = 16, 256
STATE = 3 * ACOLS
WIDE = COLS + STATE
BACK = COLS + ACOLS

CHIP_STEPS = ((1, 0), (3, 0), (2, 0), (0, 1), (1, 1), (3, 1), (2, 1))
REPLICA_STEPS = (1, 3, 2)


def call(kernel, out, flops, mib=12, **kw):
    return pl.pallas_call(
        kernel,
        out_shape=out,
        cost_estimate=pl.CostEstimate(flops=flops, bytes_accessed=4096, transcendentals=0),
        compiler_params=pltpu.CompilerParams(vmem_limit_bytes=mib * 2**20),
        **kw,
    )


def shape(dims, dtype):
    return jax.ShapeDtypeStruct(dims, dtype)


def near(*arrays):
    return [pltpu.with_memory_space_constraint(array, pltpu.VMEM) for array in arrays]


def far(*arrays):
    return [pltpu.with_memory_space_constraint(array, pltpu.HBM) for array in arrays]


def halves(x):
    high = x.astype(bf16)
    return high, (x - high.astype(f32)).astype(bf16)


def adam_update(gradient, master, moment, second, clip_factor):
    scaled = clip_factor * gradient
    moment_new = beta_one * moment + (1.0 - beta_one) * scaled
    second_new = beta_two * second + (1.0 - beta_two) * scaled * scaled
    mean_square = second_new * (1.0 / bias_two)
    root = mean_square * lax.rsqrt(mean_square)
    update = moment_new * (1.0 / bias_one) / (root + adam_eps)
    master_new = master - learn_rate * (update + weight_decay * master)
    return (master_new, moment_new, second_new)


def clip_of(sums_ref):
    total = jnp.sum(jnp.sum(sums_ref[...], axis=0, keepdims=True), axis=1, keepdims=True)
    return 1.0 / jnp.sqrt(total / NUMEL + 1e-06)


def fold_lanes(x):
    total = x[:, :128]
    for at in range(128, x.shape[1], 128):
        total = total + x[:, at : at + 128]
    return jnp.sum(total, axis=0, keepdims=True)


def pack_kernel(grad, master, moment, second, own, swap, part):
    core = lax.axis_index("gy_2")
    total = jnp.zeros((8, COLS), f32)
    for chip in range(8):
        for out, which in ((own, core), (swap, 1 - core)):
            rows = grad[2 * chip + which]
            out[chip, :, :COLS] = rows
            wide = rows.astype(f32)
            total = total + jnp.sum((wide * wide).reshape(ROWS // 8, 8, COLS), axis=0)
            cols = pl.ds(pl.multiple_of((2 * chip + which) * ACOLS, ACOLS), ACOLS)
            for n, state in enumerate((master, moment, second)):
                high, low = halves(state[:, cols])
                at = COLS + n * ACOLS
                out[chip, :AROWS, at : at + ACOLS] = high
                out[chip, AROWS:, at : at + ACOLS] = low
    part[...] = fold_lanes(total)


def route_kernel(own, swapped, *outs):
    z, x, core = (lax.axis_index(axis) for axis in GY)
    for (dz, dx), out in zip(((0, 0),) + CHIP_STEPS, outs):
        chip = lax.rem(z + dz, 4) * 2 + lax.rem(x + dx, 2)
        out[core] = own[chip]
        out[1 - core] = swapped[chip]


def sum_kernel(arrived, part, summed, copies):
    total = arrived[0].astype(f32)
    for replica in range(1, 8):
        total = total + arrived[replica].astype(f32)
    summed[...] = total
    squared = jnp.sum((total * total).reshape(32, 8, ACOLS), axis=0)
    copies[...] = jnp.broadcast_to(part[...] + fold_lanes(squared), (128, 128))


def sources():
    z, x = (lax.axis_index(axis) for axis in GY[:2])
    return [
        lax.rem(z + 4 - dz, 4) * 2 + lax.rem(x + dx, 2) for dz, dx in ((0, 0),) + CHIP_STEPS
    ]


def wide_cols(chip):
    return pl.ds(pl.multiple_of(chip * 2 * COLS, 2 * COLS), 2 * COLS)


def lanes(at):
    return slice(at * 128, (at + 1) * 128)


def expert_weight_kernel(sums, attn, *refs):
    blocks, master, streams, out = refs[:8], refs[8], refs[9:11], refs[11]
    held, weights, sems, out_sems = refs[12:]
    loads = []
    for n, chip in enumerate(sources()):
        loads.append(
            [
                pltpu.make_async_copy(array.at[:, wide_cols(chip)], held.at[m, n], sems.at[n, m])
                for m, array in enumerate(streams)
            ]
        )
        for copy in loads[n]:
            copy.start()
    clip = clip_of(sums)
    stores = []
    for n, (chip, block) in enumerate(zip(sources(), blocks)):
        for core in range(2):
            rows = pl.ds(pl.multiple_of((chip * 2 + core) * AROWS, AROWS), AROWS)
            high, low = halves(attn[rows, :])
            weights[n, core, :AROWS, COLS:] = high
            weights[n, core, AROWS:, COLS:] = low
        for copy in loads[n]:
            copy.wait()
        for at in range(14):
            core, col = divmod(at, 7)
            here = pl.ds(pl.multiple_of((chip * 14 + at) * 128, 128), 128)
            new, _, _ = adam_update(
                block[core, :, lanes(col)].astype(f32),
                master[:, here],
                held[0, n, :, lanes(at)],
                held[1, n, :, lanes(at)],
                clip,
            )
            weights[n, core, :, lanes(col)] = new.astype(bf16)
        store = pltpu.make_async_copy(weights.at[n], out.at[pl.ds(chip * 2, 2)], out_sems.at[n])
        store.start()
        stores.append(store)
    for store in stores:
        store.wait()


def expert_state_kernel(sums, *refs):
    blocks, state, outs = refs[:8], refs[8:11], refs[11:14]
    held, grads, news, sems, out_sems = refs[14:]
    loads = []
    for n, (chip, block) in enumerate(zip(sources(), blocks)):
        copies = [pltpu.make_async_copy(block.at[:, :, :COLS], grads.at[n], sems.at[n, 3])]
        for m, array in enumerate(state):
            copies.append(
                pltpu.make_async_copy(array.at[:, wide_cols(chip)], held.at[m, n], sems.at[n, m])
            )
        for copy in copies:
            copy.start()
        loads.append(copies)
    clip = clip_of(sums)
    stores = []
    for n, chip in enumerate(sources()):
        for copy in loads[n]:
            copy.wait()
        for at in range(14):
            core, col = divmod(at, 7)
            results = adam_update(
                grads[n, core, :, lanes(col)].astype(f32),
                held[0, n, :, lanes(at)],
                held[1, n, :, lanes(at)],
                held[2, n, :, lanes(at)],
                clip,
            )
            for m, result in enumerate(results):
                news[m, n, :, lanes(at)] = result
        for m, out in enumerate(outs):
            store = pltpu.make_async_copy(
                news.at[m, n], out.at[:, wide_cols(chip)], out_sems.at[n, m]
            )
            store.start()
            stores.append(store)
    for store in stores:
        store.wait()


def attn_weight_kernel(sums, attn, *refs):
    blocks, out = refs[:8], refs[8]
    clip = clip_of(sums)
    for chip, block in zip(sources(), blocks):
        for core in range(2):
            rows = pl.ds(pl.multiple_of((chip * 2 + core) * AROWS, AROWS), AROWS)
            state = block[core, :AROWS, COLS:].astype(f32) + block[core, AROWS:, COLS:].astype(f32)
            new, _, _ = adam_update(
                attn[rows, :],
                state[:, :ACOLS],
                state[:, ACOLS : 2 * ACOLS],
                state[:, 2 * ACOLS :],
                clip,
            )
            out[rows, :] = new.astype(bf16)


def both_kernel(own, other, out):
    x = lax.axis_index("gx_0")
    out[x] = own[...]
    out[1 - x] = other[...]


def finish_kernel(sums, arrived, *refs):
    pieces, state, weight, attn_weight = refs[:4], refs[4:7], refs[7], refs[8]
    outs, news, sems, out_sems = refs[9:12], refs[12], refs[13], refs[14]
    y = lax.axis_index("gx_1")
    stores = [pltpu.make_async_copy(arrived.at[:, :, :COLS], weight, sems.at[8])]
    for n, (dy, piece) in enumerate(zip((0,) + REPLICA_STEPS, pieces)):
        for x in range(2):
            slot = x * 4 + lax.rem(y + 4 - dy, 4)
            stores.append(
                pltpu.make_async_copy(piece.at[x], attn_weight.at[slot], sems.at[2 * n + x])
            )
    for store in stores:
        store.start()
    clip = clip_of(sums)
    for part in range(4):
        for group in range(4 * part, 4 * part + 4):
            cols = slice(group * ACOLS, (group + 1) * ACOLS)
            gradient = arrived[group, :AROWS, COLS:].astype(f32)
            gradient = gradient + arrived[group, AROWS:, COLS:].astype(f32)
            results = adam_update(
                gradient, state[0][:, cols], state[1][:, cols], state[2][:, cols], clip
            )
            for m, result in enumerate(results):
                news[m, :, cols] = result
        cols = pl.ds(part * 4 * ACOLS, 4 * ACOLS)
        for m, out in enumerate(outs):
            store = pltpu.make_async_copy(
                news.at[m, :, cols], out.at[:, cols], out_sems.at[part, m]
            )
            store.start()
            stores.append(store)
    for store in stores:
        store.wait()


def chip_pairs(dz, dx):
    return [(z * 2 + x, (z + dz) % 4 * 2 + (x + dx) % 2) for z in range(4) for x in range(2)]


def local(
    expert_grad,
    attn_grad,
    expert_master,
    expert_moment,
    expert_second,
    attn_master,
    attn_moment,
    attn_second,
):
    arrived = lax.all_to_all(
        attn_grad.reshape(8, 256, ACOLS), GX, split_axis=0, concat_axis=0, tiled=True
    )

    own, swap, part = call(
        pack_kernel,
        (shape((8, ROWS, WIDE), bf16), shape((8, ROWS, WIDE), bf16), shape((1, 128), f32)),
        4000000,
    )(expert_grad.reshape(16, ROWS, COLS), attn_master, attn_moment, attn_second)
    swapped = lax.ppermute(swap, "gy_2", [(0, 1), (1, 0)])
    routed = call(route_kernel, (shape((2, ROWS, WIDE), bf16),) * 8, 1000000)(own, swapped)
    blocks = [routed[0]]
    for n, step in enumerate(CHIP_STEPS):
        blocks.append(lax.ppermute(routed[n + 1], GY[:2], chip_pairs(*step)))

    attn_sum, partial = call(
        sum_kernel, (shape((256, ACOLS), f32), shape((128, 128), f32)), 2000000
    )(arrived, part)
    sums = lax.all_to_all(
        partial.reshape(128, 1, 128), GX_GY, split_axis=0, concat_axis=0, tiled=True
    ).reshape(128, 128)

    vmem = pl.BlockSpec(memory_space=pltpu.VMEM)
    hbm = pl.BlockSpec(memory_space=pltpu.HBM)
    state = far(expert_master, expert_moment, expert_second)
    attn_block = call(attn_weight_kernel, pltpu.VMEM((256, ACOLS), bf16), 2000000)(
        *near(sums, attn_sum, *blocks)
    )
    other = lax.ppermute(attn_block, "gx_0", [(0, 1), (1, 0)])
    weights = call(
        expert_weight_kernel,
        pltpu.HBM((16, ROWS, BACK), bf16),
        8000000,
        in_specs=[vmem] * 11 + [hbm] * 2,
        out_specs=hbm,
        scratch_shapes=[
            pltpu.VMEM((2, 8, ROWS, 2 * COLS), f32),
            pltpu.VMEM((8, 2, ROWS, BACK), bf16),
            pltpu.SemaphoreType.DMA((8, 2)),
            pltpu.SemaphoreType.DMA((8,)),
        ],
    )(*near(sums, attn_sum, *blocks, expert_master), *far(expert_moment, expert_second))
    returned = lax.all_to_all(weights, GY, split_axis=0, concat_axis=0, tiled=True)
    both = call(both_kernel, pltpu.VMEM((2, 256, ACOLS), bf16), 1000000)(*near(attn_block, other))
    pieces = [both]
    for n in range(3):
        pieces.append(
            lax.ppermute(both, "gx_1", [(y, (y + REPLICA_STEPS[n]) % 4) for y in range(4)])
        )
    e_master, e_moment, e_second = call(
        expert_state_kernel,
        (pltpu.HBM((ROWS, 16 * COLS), f32),) * 3,
        8000000,
        mib=16,
        in_specs=[vmem] + [hbm] * 11,
        out_specs=[hbm] * 3,
        scratch_shapes=[
            pltpu.VMEM((3, 8, ROWS, 2 * COLS), f32),
            pltpu.VMEM((8, 2, ROWS, COLS), bf16),
            pltpu.VMEM((3, 8, ROWS, 2 * COLS), f32),
            pltpu.SemaphoreType.DMA((8, 4)),
            pltpu.SemaphoreType.DMA((8, 3)),
        ],
    )(sums, *far(*blocks), *state)
    expert_weight, attn_weight, a_master, a_moment, a_second = call(
        finish_kernel,
        (pltpu.HBM((16, ROWS, COLS), bf16), pltpu.HBM((8, 256, ACOLS), bf16))
        + (pltpu.HBM((AROWS, 16 * ACOLS), f32),) * 3,
        2000000,
        in_specs=[vmem] * 9,
        out_specs=[hbm] * 5,
        scratch_shapes=[
            pltpu.VMEM((3, AROWS, 16 * ACOLS), f32),
            pltpu.SemaphoreType.DMA((9,)),
            pltpu.SemaphoreType.DMA((4, 3)),
        ],
    )(*near(sums, returned, *pieces), attn_master, attn_moment, attn_second)
    return (
        e_master,
        e_moment,
        e_second,
        a_master,
        a_moment,
        a_second,
        expert_weight.reshape(1, 16 * ROWS, COLS),
        attn_weight.reshape(2048, ACOLS),
    )


def solution(mesh):
    split = Mesh(mesh.devices.reshape(2, 4, 4, 2, 2), GX_GY)
    placed = (P(GX, None, GY),) * 2 + (P(GX_GY, None),) * 6

    return jax.shard_map(
        local,
        mesh=split,
        in_specs=placed,
        out_specs=(P(GX_GY, None),) * 6 + (P(GX, None, GY), P(None, GY)),
        check_vma=False,
    )
```

```python
import jax
import jax.numpy as jnp
from jax import lax
from jax.experimental import pallas as pl
from jax.experimental.pallas import tpu as pltpu
from jax.sharding import Mesh
from jax.sharding import PartitionSpec as P


NUMEL = 67108864
GY = ("gy_0", "gy_1", "gy_2")
GX = ("gx_0", "gx_1")
GX_GY = ("gx_0", "gx_1", "gy_0", "gy_1", "gy_2")
bf16 = jnp.bfloat16
f32 = jnp.float32

beta_one = 0.9
beta_two = 0.95
learn_rate = 0.01
weight_decay = 0.1
adam_eps = 1e-08
bias_one = 1.0 - 0.9**20
bias_two = 1.0 - 0.95**20

ROWS, COLS = 32, 896
AROWS, ACOLS = 16, 256
STATE = 3 * ACOLS
WIDE = COLS + STATE
BACK = COLS + ACOLS

CHIP_STEPS = ((1, 0), (3, 0), (2, 0), (0, 1), (1, 1), (3, 1), (2, 1))
REPLICA_STEPS = (1, 3, 2)


def call(kernel, out, flops, mib=12, **kw):
    return pl.pallas_call(
        kernel,
        out_shape=out,
        cost_estimate=pl.CostEstimate(flops=flops, bytes_accessed=4096, transcendentals=0),
        compiler_params=pltpu.CompilerParams(vmem_limit_bytes=mib * 2**20),
        **kw,
    )


def shape(dims, dtype):
    return jax.ShapeDtypeStruct(dims, dtype)


def near(*arrays):
    return [pltpu.with_memory_space_constraint(array, pltpu.VMEM) for array in arrays]


def far(*arrays):
    return [pltpu.with_memory_space_constraint(array, pltpu.HBM) for array in arrays]


def halves(x):
    high = x.astype(bf16)
    return high, (x - high.astype(f32)).astype(bf16)


def adam_update(gradient, master, moment, second, clip_factor):
    moment_new = beta_one * moment + ((1.0 - beta_one) * clip_factor) * gradient
    second_new = beta_two * second + ((1.0 - beta_two) * clip_factor * clip_factor) * (gradient * gradient)
    mean_square = second_new * (1.0 / bias_two)
    root = mean_square * lax.rsqrt(mean_square)
    step = moment_new * (learn_rate / bias_one) / (root + adam_eps)
    return (master * (1.0 - learn_rate * weight_decay) - step, moment_new, second_new)


def adam_weight(gradient, master, moment, second, clip_factor):
    gain = ((1.0 - beta_two) / bias_two) * clip_factor * clip_factor
    mean_square = (beta_two / bias_two) * second + gain * (gradient * gradient)
    root = mean_square * lax.rsqrt(mean_square)
    scale = learn_rate / bias_one
    step = (scale * beta_one) * moment + (scale * (1.0 - beta_one) * clip_factor) * gradient
    return master * (1.0 - learn_rate * weight_decay) - step / (root + adam_eps)


def clip_of(sums_ref):
    total = jnp.sum(jnp.sum(sums_ref[...], axis=0, keepdims=True), axis=1, keepdims=True)
    return 1.0 / jnp.sqrt(total / NUMEL + 1e-06)


def fold_lanes(x):
    total = x[:, :128]
    for at in range(128, x.shape[1], 128):
        total = total + x[:, at : at + 128]
    return jnp.sum(total, axis=0, keepdims=True)


def pack_kernel(grad, master, moment, second, own, swap, part):
    core = lax.axis_index("gy_2")
    total = jnp.zeros((8, COLS), f32)
    for chip in range(8):
        for out, which in ((own, core), (swap, 1 - core)):
            rows = grad[2 * chip + which]
            out[chip, :, :COLS] = rows
            wide = rows.astype(f32)
            total = total + jnp.sum((wide * wide).reshape(ROWS // 8, 8, COLS), axis=0)
            cols = pl.ds(pl.multiple_of((2 * chip + which) * ACOLS, ACOLS), ACOLS)
            for n, state in enumerate((master, moment, second)):
                high, low = halves(state[:, cols])
                at = COLS + n * ACOLS
                out[chip, :AROWS, at : at + ACOLS] = high
                out[chip, AROWS:, at : at + ACOLS] = low
    part[...] = fold_lanes(total)


def route_kernel(own, swapped, *outs):
    z, x, core = (lax.axis_index(axis) for axis in GY)
    for (dz, dx), out in zip(((0, 0),) + CHIP_STEPS, outs):
        chip = lax.rem(z + dz, 4) * 2 + lax.rem(x + dx, 2)
        out[core] = own[chip]
        out[1 - core] = swapped[chip]


def sum_kernel(arrived, part, summed, copies):
    total = arrived[0].astype(f32)
    for replica in range(1, 8):
        total = total + arrived[replica].astype(f32)
    summed[...] = total
    squared = jnp.sum((total * total).reshape(32, 8, ACOLS), axis=0)
    copies[...] = jnp.broadcast_to(part[...] + fold_lanes(squared), (128, 128))


def sources():
    z, x = (lax.axis_index(axis) for axis in GY[:2])
    return [
        lax.rem(z + 4 - dz, 4) * 2 + lax.rem(x + dx, 2) for dz, dx in ((0, 0),) + CHIP_STEPS
    ]


def wide_cols(chip):
    return pl.ds(pl.multiple_of(chip * 2 * COLS, 2 * COLS), 2 * COLS)


def lanes(at):
    return slice(at * 128, (at + 1) * 128)


def expert_weight_kernel(sums, attn, *refs):
    blocks, streams, out = refs[:8], refs[8:11], refs[11]
    held, weights, sems, out_sems = refs[12:]
    loads = []
    for n, chip in enumerate(sources()):
        loads.append(
            [
                pltpu.make_async_copy(array.at[:, wide_cols(chip)], held.at[m, n], sems.at[n, m])
                for m, array in enumerate(streams)
            ]
        )
        for copy in loads[n]:
            copy.start()
    clip = clip_of(sums)
    stores = []
    for n, (chip, block) in enumerate(zip(sources(), blocks)):
        for core in range(2):
            rows = pl.ds(pl.multiple_of((chip * 2 + core) * AROWS, AROWS), AROWS)
            high, low = halves(attn[rows, :])
            weights[n, core, :AROWS, COLS:] = high
            weights[n, core, AROWS:, COLS:] = low
        for copy in loads[n]:
            copy.wait()
        for at in range(14):
            core, col = divmod(at, 7)
            new = adam_weight(
                block[core, :, lanes(col)].astype(f32),
                held[0, n, :, lanes(at)],
                held[1, n, :, lanes(at)],
                held[2, n, :, lanes(at)],
                clip,
            )
            weights[n, core, :, lanes(col)] = new.astype(bf16)
        store = pltpu.make_async_copy(weights.at[n], out.at[pl.ds(chip * 2, 2)], out_sems.at[n])
        store.start()
        stores.append(store)
    for store in stores:
        store.wait()


def expert_state_kernel(sums, *refs):
    blocks, state, outs = refs[:8], refs[8:11], refs[11:14]
    held, grads, news, sems, out_sems = refs[14:]
    loads = []
    for n, (chip, block) in enumerate(zip(sources(), blocks)):
        copies = [pltpu.make_async_copy(block.at[:, :, :COLS], grads.at[n], sems.at[n, 3])]
        for m, array in enumerate(state):
            copies.append(
                pltpu.make_async_copy(array.at[:, wide_cols(chip)], held.at[m, n], sems.at[n, m])
            )
        for copy in copies:
            copy.start()
        loads.append(copies)
    clip = clip_of(sums)
    stores = []
    for n, chip in enumerate(sources()):
        for copy in loads[n]:
            copy.wait()
        for at in range(14):
            core, col = divmod(at, 7)
            results = adam_update(
                grads[n, core, :, lanes(col)].astype(f32),
                held[0, n, :, lanes(at)],
                held[1, n, :, lanes(at)],
                held[2, n, :, lanes(at)],
                clip,
            )
            for m, result in enumerate(results):
                news[m, n, :, lanes(at)] = result
        for m, out in enumerate(outs):
            store = pltpu.make_async_copy(
                news.at[m, n], out.at[:, wide_cols(chip)], out_sems.at[n, m]
            )
            store.start()
            stores.append(store)
    for store in stores:
        store.wait()


def attn_weight_kernel(sums, attn, *refs):
    blocks, out = refs[:8], refs[8]
    clip = clip_of(sums)
    for chip, block in zip(sources(), blocks):
        for core in range(2):
            rows = pl.ds(pl.multiple_of((chip * 2 + core) * AROWS, AROWS), AROWS)
            state = block[core, :AROWS, COLS:].astype(f32) + block[core, AROWS:, COLS:].astype(f32)
            new = adam_weight(
                attn[rows, :],
                state[:, :ACOLS],
                state[:, ACOLS : 2 * ACOLS],
                state[:, 2 * ACOLS :],
                clip,
            )
            out[rows, :] = new.astype(bf16)


def both_kernel(own, other, out):
    x = lax.axis_index("gx_0")
    out[x] = own[...]
    out[1 - x] = other[...]


def join_kernel(*refs):
    pieces, out, sems = refs[:4], refs[4], refs[5]
    y = lax.axis_index("gx_1")
    stores = []
    for n, (dy, piece) in enumerate(zip((0,) + REPLICA_STEPS, pieces)):
        for x in range(2):
            slot = x * 4 + lax.rem(y + 4 - dy, 4)
            stores.append(pltpu.make_async_copy(piece.at[x], out.at[slot], sems.at[n, x]))
            stores[-1].start()
    for store in stores:
        store.wait()


def finish_kernel(sums, arrived, *refs):
    state, weight, outs, news, sem, out_sems = refs[:3], refs[3], refs[4:7], refs[7], refs[8], refs[9]
    stores = [pltpu.make_async_copy(arrived.at[:, :, :COLS], weight, sem)]
    stores[0].start()
    clip = clip_of(sums)
    for part in range(4):
        for group in range(4 * part, 4 * part + 4):
            cols = slice(group * ACOLS, (group + 1) * ACOLS)
            gradient = arrived[group, :AROWS, COLS:].astype(f32)
            gradient = gradient + arrived[group, AROWS:, COLS:].astype(f32)
            results = adam_update(
                gradient, state[0][:, cols], state[1][:, cols], state[2][:, cols], clip
            )
            for m, result in enumerate(results):
                news[m, :, cols] = result
        cols = pl.ds(part * 4 * ACOLS, 4 * ACOLS)
        for m, out in enumerate(outs):
            store = pltpu.make_async_copy(
                news.at[m, :, cols], out.at[:, cols], out_sems.at[part, m]
            )
            store.start()
            stores.append(store)
    for store in stores:
        store.wait()


def chip_pairs(dz, dx):
    return [(z * 2 + x, (z + dz) % 4 * 2 + (x + dx) % 2) for z in range(4) for x in range(2)]


def local(
    expert_grad,
    attn_grad,
    expert_master,
    expert_moment,
    expert_second,
    attn_master,
    attn_moment,
    attn_second,
):
    arrived = lax.all_to_all(
        attn_grad.reshape(8, 256, ACOLS), GX, split_axis=0, concat_axis=0, tiled=True
    )

    own, swap, part = call(
        pack_kernel,
        (shape((8, ROWS, WIDE), bf16), shape((8, ROWS, WIDE), bf16), shape((1, 128), f32)),
        4000000,
    )(expert_grad.reshape(16, ROWS, COLS), attn_master, attn_moment, attn_second)
    swapped = lax.ppermute(swap, "gy_2", [(0, 1), (1, 0)])
    routed = call(route_kernel, (shape((2, ROWS, WIDE), bf16),) * 8, 1000000)(own, swapped)
    blocks = [routed[0]]
    for n, step in enumerate(CHIP_STEPS):
        blocks.append(lax.ppermute(routed[n + 1], GY[:2], chip_pairs(*step)))

    attn_sum, partial = call(
        sum_kernel, (shape((256, ACOLS), f32), shape((128, 128), f32)), 2000000
    )(arrived, part)
    sums = lax.all_to_all(
        partial.reshape(128, 1, 128), GX_GY, split_axis=0, concat_axis=0, tiled=True
    ).reshape(128, 128)

    vmem = pl.BlockSpec(memory_space=pltpu.VMEM)
    hbm = pl.BlockSpec(memory_space=pltpu.HBM)
    state = far(expert_master, expert_moment, expert_second)
    attn_block = call(attn_weight_kernel, pltpu.VMEM((256, ACOLS), bf16), 2000000)(
        *near(sums, attn_sum, *blocks)
    )
    other = lax.ppermute(attn_block, "gx_0", [(0, 1), (1, 0)])
    weights = call(
        expert_weight_kernel,
        pltpu.HBM((16, ROWS, BACK), bf16),
        8000000,
        in_specs=[vmem] * 10 + [hbm] * 3,
        out_specs=hbm,
        scratch_shapes=[
            pltpu.VMEM((3, 8, ROWS, 2 * COLS), f32),
            pltpu.VMEM((8, 2, ROWS, BACK), bf16),
            pltpu.SemaphoreType.DMA((8, 3)),
            pltpu.SemaphoreType.DMA((8,)),
        ],
    )(*near(sums, attn_sum, *blocks), *state)
    returned = lax.all_to_all(weights, GY, split_axis=0, concat_axis=0, tiled=True)
    both = call(both_kernel, pltpu.VMEM((2, 256, ACOLS), bf16), 1000000)(*near(attn_block, other))
    pieces = [both]
    for n in range(3):
        pieces.append(
            lax.ppermute(both, "gx_1", [(y, (y + REPLICA_STEPS[n]) % 4) for y in range(4)])
        )
    e_master, e_moment, e_second = call(
        expert_state_kernel,
        (pltpu.HBM((ROWS, 16 * COLS), f32),) * 3,
        8000000,
        mib=16,
        in_specs=[vmem] + [pl.BlockSpec(memory_space=pl.ANY)] * 8 + [hbm] * 3,
        out_specs=[hbm] * 3,
        scratch_shapes=[
            pltpu.VMEM((3, 8, ROWS, 2 * COLS), f32),
            pltpu.VMEM((8, 2, ROWS, COLS), bf16),
            pltpu.VMEM((3, 8, ROWS, 2 * COLS), f32),
            pltpu.SemaphoreType.DMA((8, 4)),
            pltpu.SemaphoreType.DMA((8, 3)),
        ],
    )(sums, *blocks, *state)
    attn_weight = call(
        join_kernel,
        pltpu.HBM((8, 256, ACOLS), bf16),
        1000000,
        in_specs=[vmem] * 4,
        out_specs=hbm,
        scratch_shapes=[pltpu.SemaphoreType.DMA((4, 2))],
    )(*near(*pieces))
    expert_weight, a_master, a_moment, a_second = call(
        finish_kernel,
        (pltpu.HBM((16, ROWS, COLS), bf16),) + (pltpu.HBM((AROWS, 16 * ACOLS), f32),) * 3,
        2000000,
        in_specs=[vmem] * 5,
        out_specs=[hbm] * 4,
        scratch_shapes=[
            pltpu.VMEM((3, AROWS, 16 * ACOLS), f32),
            pltpu.SemaphoreType.DMA,
            pltpu.SemaphoreType.DMA((4, 3)),
        ],
    )(*near(sums, returned), attn_master, attn_moment, attn_second)
    return (
        e_master,
        e_moment,
        e_second,
        a_master,
        a_moment,
        a_second,
        expert_weight.reshape(1, 16 * ROWS, COLS),
        attn_weight.reshape(2048, ACOLS),
    )


def solution(mesh):
    split = Mesh(mesh.devices.reshape(2, 4, 4, 2, 2), GX_GY)
    placed = (P(GX, None, GY),) * 2 + (P(GX_GY, None),) * 6

    return jax.shard_map(
        local,
        mesh=split,
        in_specs=placed,
        out_specs=(P(GX_GY, None),) * 6 + (P(GX, None, GY), P(None, GY)),
        check_vma=False,
    )
```

```python
import jax
import jax.numpy as jnp
from jax import lax
from jax.experimental import pallas as pl
from jax.experimental.pallas import tpu as pltpu
from jax.sharding import Mesh
from jax.sharding import PartitionSpec as P


NUMEL = 67108864
GY = ("gy_0", "gy_1", "gy_2")
GX = ("gx_0", "gx_1")
GX_GY = ("gx_0", "gx_1", "gy_0", "gy_1", "gy_2")
bf16 = jnp.bfloat16
f32 = jnp.float32

beta_one = 0.9
beta_two = 0.95
learn_rate = 0.01
weight_decay = 0.1
adam_eps = 1e-08
bias_one = 1.0 - 0.9**20
bias_two = 1.0 - 0.95**20

ROWS, COLS = 32, 896
AROWS, ACOLS = 16, 256
STATE = 3 * ACOLS
WIDE = COLS + STATE
BACK = COLS + ACOLS // 2
EARLY = 1
SHIFT = 5.2

CHIP_STEPS = ((1, 0), (3, 0), (2, 0), (0, 1), (1, 1), (3, 1), (2, 1))
REPLICA_STEPS = (1, 3, 2)


def call(kernel, out, flops, mib=12, **kw):
    return pl.pallas_call(
        kernel,
        out_shape=out,
        cost_estimate=pl.CostEstimate(flops=flops, bytes_accessed=4096, transcendentals=0),
        compiler_params=pltpu.CompilerParams(vmem_limit_bytes=mib * 2**20),
        **kw,
    )


def shape(dims, dtype):
    return jax.ShapeDtypeStruct(dims, dtype)


def near(*arrays):
    return [pltpu.with_memory_space_constraint(array, pltpu.VMEM) for array in arrays]


def far(*arrays):
    return [pltpu.with_memory_space_constraint(array, pltpu.HBM) for array in arrays]


def halves(x):
    high = x.astype(bf16)
    return high, (x - high.astype(f32)).astype(bf16)


def code(x):
    size = jnp.exp(6.0 * (jnp.log(jnp.maximum(jnp.abs(x), 1e-30)) + SHIFT))
    return jnp.where(x < 0.0, -size, size).astype(bf16)


def decode(y):
    y = y.astype(f32)
    size = jnp.exp(jnp.log(jnp.maximum(jnp.abs(y), 1e-37)) * (1.0 / 6.0) - SHIFT)
    return jnp.where(y == 0.0, 0.0, jnp.where(y < 0.0, -size, size))


def adam_update(gradient, master, moment, second, clip_factor):
    moment_new = beta_one * moment + ((1.0 - beta_one) * clip_factor) * gradient
    second_new = beta_two * second + ((1.0 - beta_two) * clip_factor * clip_factor) * (gradient * gradient)
    mean_square = second_new * (1.0 / bias_two)
    root = mean_square * lax.rsqrt(mean_square)
    step = moment_new * (learn_rate / bias_one) / (root + adam_eps)
    return (master * (1.0 - learn_rate * weight_decay) - step, moment_new, second_new)


def adam_weight(gradient, master, moment, second, clip_factor):
    gain = ((1.0 - beta_two) / bias_two) * clip_factor * clip_factor
    mean_square = (beta_two / bias_two) * second + gain * (gradient * gradient)
    root = mean_square * lax.rsqrt(mean_square)
    scale = learn_rate / bias_one
    step = (scale * beta_one) * moment + (scale * (1.0 - beta_one) * clip_factor) * gradient
    return master * (1.0 - learn_rate * weight_decay) - step / (root + adam_eps)


def clip_of(sums_ref):
    total = jnp.sum(jnp.sum(sums_ref[...], axis=0, keepdims=True), axis=1, keepdims=True)
    return 1.0 / jnp.sqrt(total / NUMEL + 1e-06)


def fold_lanes(x):
    total = x[:, :128]
    for at in range(128, x.shape[1], 128):
        total = total + x[:, at : at + 128]
    return jnp.sum(total, axis=0, keepdims=True)


def pack_kernel(grad, master, moment, second, own, swap, part):
    core = lax.axis_index("gy_2")
    total = jnp.zeros((8, COLS), f32)
    for chip in range(8):
        for out, which in ((own, core), (swap, 1 - core)):
            rows = grad[2 * chip + which]
            out[chip, :, :COLS] = rows
            wide = rows.astype(f32)
            total = total + jnp.sum((wide * wide).reshape(ROWS // 8, 8, COLS), axis=0)
            cols = pl.ds(pl.multiple_of((2 * chip + which) * ACOLS, ACOLS), ACOLS)
            for n, state in enumerate((master, moment, second)):
                high, low = halves(state[:, cols])
                at = COLS + n * ACOLS
                out[chip, :AROWS, at : at + ACOLS] = high
                out[chip, AROWS:, at : at + ACOLS] = low
    part[...] = fold_lanes(total)


def route_kernel(own, swapped, *outs):
    z, x, core = (lax.axis_index(axis) for axis in GY)
    for (dz, dx), out in zip(((0, 0),) + CHIP_STEPS, outs):
        chip = lax.rem(z + dz, 4) * 2 + lax.rem(x + dx, 2)
        out[core] = own[chip]
        out[1 - core] = swapped[chip]


def sum_kernel(arrived, part, summed, copies):
    total = arrived[0].astype(f32)
    for replica in range(1, 8):
        total = total + arrived[replica].astype(f32)
    summed[...] = total
    squared = jnp.sum((total * total).reshape(32, 8, ACOLS), axis=0)
    copies[...] = jnp.broadcast_to(part[...] + fold_lanes(squared), (128, 128))


def sources():
    z, x = (lax.axis_index(axis) for axis in GY[:2])
    return [
        lax.rem(z + 4 - dz, 4) * 2 + lax.rem(x + dx, 2) for dz, dx in ((0, 0),) + CHIP_STEPS
    ]


def wide_cols(chip):
    return pl.ds(pl.multiple_of(chip * 2 * COLS, 2 * COLS), 2 * COLS)


def lanes(at):
    return slice(at * 128, (at + 1) * 128)


def expert_weight_kernel(sums, attn, *refs):
    blocks, early, streams, out = refs[:8], refs[8], refs[9:12], refs[12]
    held, weights, sems, out_sems = refs[13:]
    loads = []
    for n, chip in enumerate(sources()):
        loads.append(
            [
                pltpu.make_async_copy(array.at[:, wide_cols(chip)], held.at[m, n - EARLY], sems.at[n - EARLY, m])
                for m, array in enumerate(streams)
                if n >= EARLY
            ]
        )
        for copy in loads[n]:
            copy.start()
    clip = clip_of(sums)
    stores = []
    for n, (chip, block) in enumerate(zip(sources(), blocks)):
        for core in range(2):
            rows = pl.ds(pl.multiple_of((chip * 2 + core) * AROWS, AROWS), AROWS)
            scaled = code(clip * attn[rows, :])
            weights[n, core, :AROWS, COLS:] = scaled[:, :128]
            weights[n, core, AROWS:, COLS:] = scaled[:, 128:]
        for copy in loads[n]:
            copy.wait()
        state = early.at[:, n] if n < EARLY else held.at[:, n - EARLY]
        for at in range(14):
            core, col = divmod(at, 7)
            new = adam_weight(
                block[core, :, lanes(col)].astype(f32),
                state[0, :, lanes(at)],
                state[1, :, lanes(at)],
                state[2, :, lanes(at)],
                clip,
            )
            weights[n, core, :, lanes(col)] = new.astype(bf16)
        store = pltpu.make_async_copy(weights.at[n], out.at[pl.ds(chip * 2, 2)], out_sems.at[n])
        store.start()
        stores.append(store)
    for store in stores:
        store.wait()


def expert_state_kernel(sums, *refs):
    blocks, state, outs = refs[:8], refs[8:11], refs[11:14]
    held, grads, news, sems, out_sems = refs[14:]
    loads = []
    for n, (chip, block) in enumerate(zip(sources(), blocks)):
        copies = [pltpu.make_async_copy(block.at[:, :, :COLS], grads.at[n], sems.at[n, 3])]
        for m, array in enumerate(state):
            copies.append(
                pltpu.make_async_copy(array.at[:, wide_cols(chip)], held.at[m, n], sems.at[n, m])
            )
        for copy in copies:
            copy.start()
        loads.append(copies)
    clip = clip_of(sums)
    stores = []
    for n, chip in enumerate(sources()):
        for copy in loads[n]:
            copy.wait()
        for at in range(14):
            core, col = divmod(at, 7)
            results = adam_update(
                grads[n, core, :, lanes(col)].astype(f32),
                held[0, n, :, lanes(at)],
                held[1, n, :, lanes(at)],
                held[2, n, :, lanes(at)],
                clip,
            )
            for m, result in enumerate(results):
                news[m, n, :, lanes(at)] = result
        for m, out in enumerate(outs):
            store = pltpu.make_async_copy(
                news.at[m, n], out.at[:, wide_cols(chip)], out_sems.at[n, m]
            )
            store.start()
            stores.append(store)
    for store in stores:
        store.wait()


def attn_weight_kernel(sums, attn, *refs):
    blocks, state, out, early, sems = refs[:8], refs[8:11], refs[11], refs[12], refs[13]
    loads = []
    for n, chip in enumerate(sources()[:EARLY]):
        for m, array in enumerate(state):
            loads.append(
                pltpu.make_async_copy(array.at[:, wide_cols(chip)], early.at[m, n], sems.at[n, m])
            )
            loads[-1].start()
    clip = clip_of(sums)
    for chip, block in zip(sources(), blocks):
        for core in range(2):
            rows = pl.ds(pl.multiple_of((chip * 2 + core) * AROWS, AROWS), AROWS)
            came = block[core, :AROWS, COLS:].astype(f32) + block[core, AROWS:, COLS:].astype(f32)
            new = adam_weight(
                attn[rows, :],
                came[:, :ACOLS],
                came[:, ACOLS : 2 * ACOLS],
                came[:, 2 * ACOLS :],
                clip,
            )
            out[rows, :] = new.astype(bf16)
    for copy in loads:
        copy.wait()


def join_kernel(*refs):
    out, sems = refs[8], refs[9]
    x, y = (lax.axis_index(axis) for axis in GX)
    stores = []
    for half, row in enumerate((x, 1 - x)):
        for n, dy in enumerate((0,) + REPLICA_STEPS):
            slot = row * 4 + lax.rem(y + 4 - dy, 4)
            at = 4 * half + n
            stores.append(pltpu.make_async_copy(refs[at], out.at[slot], sems.at[at]))
            stores[-1].start()
    for store in stores:
        store.wait()


def finish_kernel(arrived, *refs):
    state, weight, outs, news, sem, out_sems = refs[:3], refs[3], refs[4:7], refs[7], refs[8], refs[9]
    stores = [pltpu.make_async_copy(arrived.at[:, :, :COLS], weight, sem)]
    stores[0].start()
    for part in range(4):
        for group in range(4 * part, 4 * part + 4):
            for half in range(2):
                scaled = decode(arrived[group, half * AROWS : (half + 1) * AROWS, COLS:])
                cols = lanes(2 * group + half)
                results = adam_update(
                    scaled, state[0][:, cols], state[1][:, cols], state[2][:, cols], 1.0
                )
                for m, result in enumerate(results):
                    news[m, :, cols] = result
        cols = pl.ds(part * 4 * ACOLS, 4 * ACOLS)
        for m, out in enumerate(outs):
            store = pltpu.make_async_copy(
                news.at[m, :, cols], out.at[:, cols], out_sems.at[part, m]
            )
            store.start()
            stores.append(store)
    for store in stores:
        store.wait()


def chip_pairs(dz, dx):
    return [(z * 2 + x, (z + dz) % 4 * 2 + (x + dx) % 2) for z in range(4) for x in range(2)]


def local(
    expert_grad,
    attn_grad,
    expert_master,
    expert_moment,
    expert_second,
    attn_master,
    attn_moment,
    attn_second,
):
    arrived = lax.all_to_all(
        attn_grad.reshape(8, 256, ACOLS), GX, split_axis=0, concat_axis=0, tiled=True
    )

    own, swap, part = call(
        pack_kernel,
        (shape((8, ROWS, WIDE), bf16), shape((8, ROWS, WIDE), bf16), shape((1, 128), f32)),
        4000000,
    )(expert_grad.reshape(16, ROWS, COLS), attn_master, attn_moment, attn_second)
    swapped = lax.ppermute(swap, "gy_2", [(0, 1), (1, 0)])
    routed = call(route_kernel, (shape((2, ROWS, WIDE), bf16),) * 8, 1000000)(own, swapped)
    blocks = [routed[0]]
    for n, step in enumerate(CHIP_STEPS):
        blocks.append(lax.ppermute(routed[n + 1], GY[:2], chip_pairs(*step)))

    attn_sum, partial = call(
        sum_kernel, (shape((256, ACOLS), f32), shape((128, 128), f32)), 2000000
    )(arrived, part)
    sums = lax.all_to_all(
        partial.reshape(128, 1, 128), GX_GY, split_axis=0, concat_axis=0, tiled=True
    ).reshape(128, 128)

    vmem = pl.BlockSpec(memory_space=pltpu.VMEM)
    hbm = pl.BlockSpec(memory_space=pltpu.HBM)
    state = far(expert_master, expert_moment, expert_second)
    attn_block, early = call(
        attn_weight_kernel,
        (pltpu.VMEM((256, ACOLS), bf16), pltpu.VMEM((3, EARLY, ROWS, 2 * COLS), f32)),
        2000000,
        in_specs=[vmem] * 10 + [hbm] * 3,
        out_specs=[vmem] * 2,
        scratch_shapes=[pltpu.SemaphoreType.DMA((EARLY, 3))],
    )(*near(sums, attn_sum, *blocks), *state)
    other = lax.ppermute(attn_block, "gx_0", [(0, 1), (1, 0)])
    weights = call(
        expert_weight_kernel,
        pltpu.HBM((16, ROWS, BACK), bf16),
        8000000,
        in_specs=[vmem] * 11 + [hbm] * 3,
        out_specs=hbm,
        scratch_shapes=[
            pltpu.VMEM((3, 8 - EARLY, ROWS, 2 * COLS), f32),
            pltpu.VMEM((8, 2, ROWS, BACK), bf16),
            pltpu.SemaphoreType.DMA((8 - EARLY, 3)),
            pltpu.SemaphoreType.DMA((8,)),
        ],
    )(*near(sums, attn_sum, *blocks, early), *state)
    returned = lax.all_to_all(weights, GY, split_axis=0, concat_axis=0, tiled=True)
    pieces = []
    for block in (attn_block, other):
        pieces.append(block)
        for dy in REPLICA_STEPS:
            pieces.append(
                lax.ppermute(block, "gx_1", [(y, (y + dy) % 4) for y in range(4)])
            )
    e_master, e_moment, e_second = call(
        expert_state_kernel,
        (pltpu.HBM((ROWS, 16 * COLS), f32),) * 3,
        8000000,
        mib=16,
        in_specs=[vmem] + [pl.BlockSpec(memory_space=pl.ANY)] * 8 + [hbm] * 3,
        out_specs=[hbm] * 3,
        scratch_shapes=[
            pltpu.VMEM((3, 8, ROWS, 2 * COLS), f32),
            pltpu.VMEM((8, 2, ROWS, COLS), bf16),
            pltpu.VMEM((3, 8, ROWS, 2 * COLS), f32),
            pltpu.SemaphoreType.DMA((8, 4)),
            pltpu.SemaphoreType.DMA((8, 3)),
        ],
    )(sums, *blocks, *state)
    attn_weight = call(
        join_kernel,
        pltpu.HBM((8, 256, ACOLS), bf16),
        1000000,
        in_specs=[vmem] * 8,
        out_specs=hbm,
        scratch_shapes=[pltpu.SemaphoreType.DMA((8,))],
    )(*near(*pieces))
    expert_weight, a_master, a_moment, a_second = call(
        finish_kernel,
        (pltpu.HBM((16, ROWS, COLS), bf16),) + (pltpu.HBM((AROWS, 16 * ACOLS), f32),) * 3,
        2000000,
        in_specs=[vmem] * 4,
        out_specs=[hbm] * 4,
        scratch_shapes=[
            pltpu.VMEM((3, AROWS, 16 * ACOLS), f32),
            pltpu.SemaphoreType.DMA,
            pltpu.SemaphoreType.DMA((4, 3)),
        ],
    )(*near(returned), attn_master, attn_moment, attn_second)
    return (
        e_master,
        e_moment,
        e_second,
        a_master,
        a_moment,
        a_second,
        expert_weight.reshape(1, 16 * ROWS, COLS),
        attn_weight.reshape(2048, ACOLS),
    )


def solution(mesh):
    split = Mesh(mesh.devices.reshape(2, 4, 4, 2, 2), GX_GY)
    placed = (P(GX, None, GY),) * 2 + (P(GX_GY, None),) * 6

    return jax.shard_map(
        local,
        mesh=split,
        in_specs=placed,
        out_specs=(P(GX_GY, None),) * 6 + (P(GX, None, GY), P(None, GY)),
        check_vma=False,
    )
```

```python
import jax
import jax.numpy as jnp
from jax import lax
from jax.experimental import pallas as pl
from jax.experimental.pallas import tpu as pltpu
from jax.sharding import Mesh
from jax.sharding import PartitionSpec as P


NUMEL = 67108864
GY = ("gy_0", "gy_1", "gy_2")
GX = ("gx_0", "gx_1")
GX_GY = ("gx_0", "gx_1", "gy_0", "gy_1", "gy_2")
bf16 = jnp.bfloat16
f32 = jnp.float32

beta_one = 0.9
beta_two = 0.95
learn_rate = 0.01
weight_decay = 0.1
adam_eps = 1e-08
bias_one = 1.0 - 0.9**20
bias_two = 1.0 - 0.95**20

ROWS, COLS = 32, 896
AROWS, ACOLS = 16, 256
STATE = 3 * ACOLS
WIDE = COLS + STATE
BACK = COLS + ACOLS // 2
EARLY = 1
TOP = 87.0
POWER = 12.0

CHIP_STEPS = ((1, 0), (3, 0), (2, 0), (0, 1), (1, 1), (3, 1), (2, 1))
REPLICA_STEPS = (1, 3, 2)


def call(kernel, out, flops, mib=12, **kw):
    return pl.pallas_call(
        kernel,
        out_shape=out,
        cost_estimate=pl.CostEstimate(flops=flops, bytes_accessed=4096, transcendentals=0),
        compiler_params=pltpu.CompilerParams(vmem_limit_bytes=mib * 2**20),
        **kw,
    )


def shape(dims, dtype):
    return jax.ShapeDtypeStruct(dims, dtype)


def near(*arrays):
    return [pltpu.with_memory_space_constraint(array, pltpu.VMEM) for array in arrays]


def far(*arrays):
    return [pltpu.with_memory_space_constraint(array, pltpu.HBM) for array in arrays]


def halves(x):
    high = x.astype(bf16)
    return high, (x - high.astype(f32)).astype(bf16)


def largest(x):
    return jnp.max(jnp.max(jnp.abs(x), axis=0, keepdims=True), axis=1, keepdims=True)


def code(x, most):
    size = jnp.maximum(jnp.abs(x) / jnp.where(most == 0.0, 1.0, most), 1e-30)
    size = jnp.exp(POWER * jnp.log(size) + TOP)
    return jnp.where(x < 0.0, -size, size).astype(bf16)


def decode(y, most):
    y = y.astype(f32)
    size = most * jnp.exp((jnp.log(jnp.maximum(jnp.abs(y), 1e-37)) - TOP) * (1.0 / POWER))
    return jnp.where(y == 0.0, 0.0, jnp.where(y < 0.0, -size, size))


def adam_update(gradient, master, moment, second, clip_factor):
    moment_new = beta_one * moment + ((1.0 - beta_one) * clip_factor) * gradient
    second_new = beta_two * second + ((1.0 - beta_two) * clip_factor * clip_factor) * (gradient * gradient)
    mean_square = second_new * (1.0 / bias_two)
    root = mean_square * lax.rsqrt(mean_square)
    step = moment_new * (learn_rate / bias_one) / (root + adam_eps)
    return (master * (1.0 - learn_rate * weight_decay) - step, moment_new, second_new)


def adam_weight(gradient, master, moment, second, clip_factor):
    gain = ((1.0 - beta_two) / bias_two) * clip_factor * clip_factor
    mean_square = (beta_two / bias_two) * second + gain * (gradient * gradient)
    root = mean_square * lax.rsqrt(mean_square)
    scale = learn_rate / bias_one
    step = (scale * beta_one) * moment + (scale * (1.0 - beta_one) * clip_factor) * gradient
    return master * (1.0 - learn_rate * weight_decay) - step / (root + adam_eps)


def clip_of(sums_ref):
    total = jnp.sum(sums_ref[...], axis=0, keepdims=True)
    lane = lax.broadcasted_iota(jnp.int32, (1, 128), 1)
    total = jnp.sum(jnp.where(lane < 64, total, 0.0), axis=1, keepdims=True)
    return 1.0 / jnp.sqrt(total / NUMEL + 1e-06)


def fold_lanes(x):
    total = x[:, :128]
    for at in range(128, x.shape[1], 128):
        total = total + x[:, at : at + 128]
    return jnp.sum(total, axis=0, keepdims=True)


def pack_kernel(grad, master, moment, second, own, swap, part):
    core = lax.axis_index("gy_2")
    total = jnp.zeros((8, COLS), f32)
    for chip in range(8):
        for out, which in ((own, core), (swap, 1 - core)):
            rows = grad[2 * chip + which]
            out[chip, :, :COLS] = rows
            wide = rows.astype(f32)
            total = total + jnp.sum((wide * wide).reshape(ROWS // 8, 8, COLS), axis=0)
            cols = pl.ds(pl.multiple_of((2 * chip + which) * ACOLS, ACOLS), ACOLS)
            for n, state in enumerate((master, moment, second)):
                high, low = halves(state[:, cols])
                at = COLS + n * ACOLS
                out[chip, :AROWS, at : at + ACOLS] = high
                out[chip, AROWS:, at : at + ACOLS] = low
    part[...] = fold_lanes(total)


def route_kernel(own, swapped, *outs):
    z, x, core = (lax.axis_index(axis) for axis in GY)
    for (dz, dx), out in zip(((0, 0),) + CHIP_STEPS, outs):
        chip = lax.rem(z + dz, 4) * 2 + lax.rem(x + dx, 2)
        out[core] = own[chip]
        out[1 - core] = swapped[chip]


def sum_kernel(arrived, part, summed, copies):
    total = arrived[0].astype(f32)
    for replica in range(1, 8):
        total = total + arrived[replica].astype(f32)
    summed[...] = total
    squared = jnp.sum((total * total).reshape(32, 8, ACOLS), axis=0)
    lane = lax.broadcasted_iota(jnp.int32, (1, 128), 1)
    row = part[...] + fold_lanes(squared)
    row = row + pltpu.roll(row, 64, 1)
    for group in range(16):
        top = largest(total[group * AROWS : (group + 1) * AROWS, :])
        row = jnp.where(lane == 64 + group, top, row)
    copies[...] = jnp.broadcast_to(row, (128, 128))


def sources():
    z, x = (lax.axis_index(axis) for axis in GY[:2])
    return [
        lax.rem(z + 4 - dz, 4) * 2 + lax.rem(x + dx, 2) for dz, dx in ((0, 0),) + CHIP_STEPS
    ]


def wide_cols(chip):
    return pl.ds(pl.multiple_of(chip * 2 * COLS, 2 * COLS), 2 * COLS)


def lanes(at):
    return slice(at * 128, (at + 1) * 128)


def expert_weight_kernel(sums, attn, *refs):
    blocks, early, streams, out = refs[:8], refs[8], refs[9:12], refs[12]
    held, weights, sems, out_sems = refs[13:]
    loads = []
    for n, chip in enumerate(sources()):
        loads.append(
            [
                pltpu.make_async_copy(array.at[:, wide_cols(chip)], held.at[m, n - EARLY], sems.at[n - EARLY, m])
                for m, array in enumerate(streams)
                if n >= EARLY
            ]
        )
        for copy in loads[n]:
            copy.start()
    clip = clip_of(sums)
    stores = []
    for n, (chip, block) in enumerate(zip(sources(), blocks)):
        for core in range(2):
            rows = pl.ds(pl.multiple_of((chip * 2 + core) * AROWS, AROWS), AROWS)
            summed = attn[rows, :]
            scaled = code(summed, largest(summed))
            weights[n, core, :AROWS, COLS:] = scaled[:, :128]
            weights[n, core, AROWS:, COLS:] = scaled[:, 128:]
        for copy in loads[n]:
            copy.wait()
        state = early.at[:, n] if n < EARLY else held.at[:, n - EARLY]
        for at in range(14):
            core, col = divmod(at, 7)
            new = adam_weight(
                block[core, :, lanes(col)].astype(f32),
                state[0, :, lanes(at)],
                state[1, :, lanes(at)],
                state[2, :, lanes(at)],
                clip,
            )
            weights[n, core, :, lanes(col)] = new.astype(bf16)
        store = pltpu.make_async_copy(weights.at[n], out.at[pl.ds(chip * 2, 2)], out_sems.at[n])
        store.start()
        stores.append(store)
    for store in stores:
        store.wait()


def expert_state_kernel(sums, *refs):
    blocks, state, outs = refs[:8], refs[8:11], refs[11:14]
    held, grads, news, sems, out_sems = refs[14:]
    loads = []
    for n, (chip, block) in enumerate(zip(sources(), blocks)):
        copies = [pltpu.make_async_copy(block.at[:, :, :COLS], grads.at[n], sems.at[n, 3])]
        for m, array in enumerate(state):
            copies.append(
                pltpu.make_async_copy(array.at[:, wide_cols(chip)], held.at[m, n], sems.at[n, m])
            )
        for copy in copies:
            copy.start()
        loads.append(copies)
    clip = clip_of(sums)
    stores = []
    for n, chip in enumerate(sources()):
        for copy in loads[n]:
            copy.wait()
        for at in range(14):
            core, col = divmod(at, 7)
            results = adam_update(
                grads[n, core, :, lanes(col)].astype(f32),
                held[0, n, :, lanes(at)],
                held[1, n, :, lanes(at)],
                held[2, n, :, lanes(at)],
                clip,
            )
            for m, result in enumerate(results):
                news[m, n, :, lanes(at)] = result
        for m, out in enumerate(outs):
            store = pltpu.make_async_copy(
                news.at[m, n], out.at[:, wide_cols(chip)], out_sems.at[n, m]
            )
            store.start()
            stores.append(store)
    for store in stores:
        store.wait()


def attn_weight_kernel(sums, attn, *refs):
    blocks, state, out, early, sems = refs[:8], refs[8:11], refs[11], refs[12], refs[13]
    loads = []
    for n, chip in enumerate(sources()[:EARLY]):
        for m, array in enumerate(state):
            loads.append(
                pltpu.make_async_copy(array.at[:, wide_cols(chip)], early.at[m, n], sems.at[n, m])
            )
            loads[-1].start()
    clip = clip_of(sums)
    for chip, block in zip(sources(), blocks):
        for core in range(2):
            rows = pl.ds(pl.multiple_of((chip * 2 + core) * AROWS, AROWS), AROWS)
            came = block[core, :AROWS, COLS:].astype(f32) + block[core, AROWS:, COLS:].astype(f32)
            new = adam_weight(
                attn[rows, :],
                came[:, :ACOLS],
                came[:, ACOLS : 2 * ACOLS],
                came[:, 2 * ACOLS :],
                clip,
            )
            out[rows, :] = new.astype(bf16)
    for copy in loads:
        copy.wait()


def join_kernel(*refs):
    out, sems = refs[8], refs[9]
    x, y = (lax.axis_index(axis) for axis in GX)
    stores = []
    for half, row in enumerate((x, 1 - x)):
        for n, dy in enumerate((0,) + REPLICA_STEPS):
            slot = row * 4 + lax.rem(y + 4 - dy, 4)
            at = 4 * half + n
            stores.append(pltpu.make_async_copy(refs[at], out.at[slot], sems.at[at]))
            stores[-1].start()
    for store in stores:
        store.wait()


def finish_kernel(sums, arrived, *refs):
    state, weight, outs, news, sem, out_sems = refs[:3], refs[3], refs[4:7], refs[7], refs[8], refs[9]
    stores = [pltpu.make_async_copy(arrived.at[:, :, :COLS], weight, sem)]
    stores[0].start()
    clip = clip_of(sums)
    replica = lax.axis_index("gx_0") * 4 + lax.axis_index("gx_1")
    me = lax.axis_index("gy_0") * 4 + lax.axis_index("gy_1") * 2 + lax.axis_index("gy_2")
    mine = lax.broadcasted_iota(jnp.int32, (16, 128), 1) == 64 + me
    tops = sums[pl.ds(pl.multiple_of(replica * 16, 16), 16), :]
    tops = clip * jnp.sum(jnp.where(mine, tops, 0.0), axis=1, keepdims=True)
    for part in range(4):
        for group in range(4 * part, 4 * part + 4):
            for half in range(2):
                scaled = decode(
                    arrived[group, half * AROWS : (half + 1) * AROWS, COLS:], tops[group : group + 1, :]
                )
                cols = lanes(2 * group + half)
                results = adam_update(
                    scaled, state[0][:, cols], state[1][:, cols], state[2][:, cols], 1.0
                )
                for m, result in enumerate(results):
                    news[m, :, cols] = result
        cols = pl.ds(part * 4 * ACOLS, 4 * ACOLS)
        for m, out in enumerate(outs):
            store = pltpu.make_async_copy(
                news.at[m, :, cols], out.at[:, cols], out_sems.at[part, m]
            )
            store.start()
            stores.append(store)
    for store in stores:
        store.wait()


def chip_pairs(dz, dx):
    return [(z * 2 + x, (z + dz) % 4 * 2 + (x + dx) % 2) for z in range(4) for x in range(2)]


def local(
    expert_grad,
    attn_grad,
    expert_master,
    expert_moment,
    expert_second,
    attn_master,
    attn_moment,
    attn_second,
):
    arrived = lax.all_to_all(
        attn_grad.reshape(8, 256, ACOLS), GX, split_axis=0, concat_axis=0, tiled=True
    )

    own, swap, part = call(
        pack_kernel,
        (shape((8, ROWS, WIDE), bf16), shape((8, ROWS, WIDE), bf16), shape((1, 128), f32)),
        4000000,
    )(expert_grad.reshape(16, ROWS, COLS), attn_master, attn_moment, attn_second)
    swapped = lax.ppermute(swap, "gy_2", [(0, 1), (1, 0)])
    routed = call(route_kernel, (shape((2, ROWS, WIDE), bf16),) * 8, 1000000)(own, swapped)
    blocks = [routed[0]]
    for n, step in enumerate(CHIP_STEPS):
        blocks.append(lax.ppermute(routed[n + 1], GY[:2], chip_pairs(*step)))

    attn_sum, partial = call(
        sum_kernel, (shape((256, ACOLS), f32), shape((128, 128), f32)), 2000000
    )(arrived, part)
    sums = lax.all_to_all(
        partial.reshape(128, 1, 128), GX_GY, split_axis=0, concat_axis=0, tiled=True
    ).reshape(128, 128)

    vmem = pl.BlockSpec(memory_space=pltpu.VMEM)
    hbm = pl.BlockSpec(memory_space=pltpu.HBM)
    state = far(expert_master, expert_moment, expert_second)
    attn_block, early = call(
        attn_weight_kernel,
        (pltpu.VMEM((256, ACOLS), bf16), pltpu.VMEM((3, EARLY, ROWS, 2 * COLS), f32)),
        2000000,
        in_specs=[vmem] * 10 + [hbm] * 3,
        out_specs=[vmem] * 2,
        scratch_shapes=[pltpu.SemaphoreType.DMA((EARLY, 3))],
    )(*near(sums, attn_sum, *blocks), *state)
    other = lax.ppermute(attn_block, "gx_0", [(0, 1), (1, 0)])
    weights = call(
        expert_weight_kernel,
        pltpu.HBM((16, ROWS, BACK), bf16),
        8000000,
        in_specs=[vmem] * 11 + [hbm] * 3,
        out_specs=hbm,
        scratch_shapes=[
            pltpu.VMEM((3, 8 - EARLY, ROWS, 2 * COLS), f32),
            pltpu.VMEM((8, 2, ROWS, BACK), bf16),
            pltpu.SemaphoreType.DMA((8 - EARLY, 3)),
            pltpu.SemaphoreType.DMA((8,)),
        ],
    )(*near(sums, attn_sum, *blocks, early), *state)
    returned = lax.all_to_all(weights, GY, split_axis=0, concat_axis=0, tiled=True)
    pieces = []
    for block in (attn_block, other):
        pieces.append(block)
        for dy in REPLICA_STEPS:
            pieces.append(
                lax.ppermute(block, "gx_1", [(y, (y + dy) % 4) for y in range(4)])
            )
    e_master, e_moment, e_second = call(
        expert_state_kernel,
        (pltpu.HBM((ROWS, 16 * COLS), f32),) * 3,
        8000000,
        mib=16,
        in_specs=[vmem] + [pl.BlockSpec(memory_space=pl.ANY)] * 8 + [hbm] * 3,
        out_specs=[hbm] * 3,
        scratch_shapes=[
            pltpu.VMEM((3, 8, ROWS, 2 * COLS), f32),
            pltpu.VMEM((8, 2, ROWS, COLS), bf16),
            pltpu.VMEM((3, 8, ROWS, 2 * COLS), f32),
            pltpu.SemaphoreType.DMA((8, 4)),
            pltpu.SemaphoreType.DMA((8, 3)),
        ],
    )(sums, *blocks, *state)
    attn_weight = call(
        join_kernel,
        pltpu.HBM((8, 256, ACOLS), bf16),
        1000000,
        in_specs=[vmem] * 8,
        out_specs=hbm,
        scratch_shapes=[pltpu.SemaphoreType.DMA((8,))],
    )(*near(*pieces))
    expert_weight, a_master, a_moment, a_second = call(
        finish_kernel,
        (pltpu.HBM((16, ROWS, COLS), bf16),) + (pltpu.HBM((AROWS, 16 * ACOLS), f32),) * 3,
        2000000,
        in_specs=[vmem] * 5,
        out_specs=[hbm] * 4,
        scratch_shapes=[
            pltpu.VMEM((3, AROWS, 16 * ACOLS), f32),
            pltpu.SemaphoreType.DMA,
            pltpu.SemaphoreType.DMA((4, 3)),
        ],
    )(*near(sums, returned), attn_master, attn_moment, attn_second)
    return (
        e_master,
        e_moment,
        e_second,
        a_master,
        a_moment,
        a_second,
        expert_weight.reshape(1, 16 * ROWS, COLS),
        attn_weight.reshape(2048, ACOLS),
    )


def solution(mesh):
    split = Mesh(mesh.devices.reshape(2, 4, 4, 2, 2), GX_GY)
    placed = (P(GX, None, GY),) * 2 + (P(GX_GY, None),) * 6

    return jax.shard_map(
        local,
        mesh=split,
        in_specs=placed,
        out_specs=(P(GX_GY, None),) * 6 + (P(GX, None, GY), P(None, GY)),
        check_vma=False,
    )
```

```python
import jax
import jax.numpy as jnp
from jax import lax
from jax.experimental import pallas as pl
from jax.experimental.pallas import tpu as pltpu
from jax.sharding import Mesh
from jax.sharding import PartitionSpec as P


NUMEL = 67108864
GY = ("gy_0", "gy_1", "gy_2")
GX = ("gx_0", "gx_1")
GX_GY = ("gx_0", "gx_1", "gy_0", "gy_1", "gy_2")
bf16 = jnp.bfloat16
f32 = jnp.float32

beta_one = 0.9
beta_two = 0.95
learn_rate = 0.01
weight_decay = 0.1
adam_eps = 1e-08
bias_one = 1.0 - 0.9**20
bias_two = 1.0 - 0.95**20

ROWS, COLS = 32, 896
AROWS, ACOLS = 16, 256
STATE = 2 * ACOLS + ACOLS // 2
WIDE = COLS + STATE
BACK = COLS + ACOLS // 2
EARLY = 1
TOP = 87.0
POWER = 12.0
MIDDLE = -0.458

CHIP_STEPS = ((1, 0), (3, 0), (2, 0), (0, 1), (1, 1), (3, 1), (2, 1))
REPLICA_STEPS = (1, 3, 2)


def call(kernel, out, flops, mib=12, **kw):
    return pl.pallas_call(
        kernel,
        out_shape=out,
        cost_estimate=pl.CostEstimate(flops=flops, bytes_accessed=4096, transcendentals=0),
        compiler_params=pltpu.CompilerParams(vmem_limit_bytes=mib * 2**20),
        **kw,
    )


def shape(dims, dtype):
    return jax.ShapeDtypeStruct(dims, dtype)


def near(*arrays):
    return [pltpu.with_memory_space_constraint(array, pltpu.VMEM) for array in arrays]


def far(*arrays):
    return [pltpu.with_memory_space_constraint(array, pltpu.HBM) for array in arrays]


def halves(x):
    high = x.astype(bf16)
    return high, (x - high.astype(f32)).astype(bf16)


def largest(x):
    return jnp.max(jnp.max(jnp.abs(x), axis=0, keepdims=True), axis=1, keepdims=True)


def code(x, most):
    size = jnp.maximum(jnp.abs(x) / jnp.where(most == 0.0, 1.0, most), 1e-30)
    size = jnp.exp(POWER * jnp.log(size) + TOP)
    return jnp.where(x < 0.0, -size, size).astype(bf16)


def decode(y, most):
    y = y.astype(f32)
    size = most * jnp.exp((jnp.log(jnp.maximum(jnp.abs(y), 1e-37)) - TOP) * (1.0 / POWER))
    return jnp.where(y == 0.0, 0.0, jnp.where(y < 0.0, -size, size))


def code_second(x):
    return jnp.exp(40.0 * (jnp.log(x) - MIDDLE)).astype(bf16)


def decode_second(y):
    return jnp.exp(jnp.log(y.astype(f32)) * (1.0 / 40.0) + MIDDLE)


def adam_update(gradient, master, moment, second, clip_factor):
    moment_new = beta_one * moment + ((1.0 - beta_one) * clip_factor) * gradient
    second_new = beta_two * second + ((1.0 - beta_two) * clip_factor * clip_factor) * (gradient * gradient)
    mean_square = second_new * (1.0 / bias_two)
    root = mean_square * lax.rsqrt(mean_square)
    step = moment_new * (learn_rate / bias_one) / (root + adam_eps)
    return (master * (1.0 - learn_rate * weight_decay) - step, moment_new, second_new)


def adam_weight(gradient, master, moment, second, clip_factor):
    gain = ((1.0 - beta_two) / bias_two) * clip_factor * clip_factor
    mean_square = (beta_two / bias_two) * second + gain * (gradient * gradient)
    root = mean_square * lax.rsqrt(mean_square)
    scale = learn_rate / bias_one
    step = (scale * beta_one) * moment + (scale * (1.0 - beta_one) * clip_factor) * gradient
    return master * (1.0 - learn_rate * weight_decay) - step / (root + adam_eps)


def clip_of(sums_ref):
    total = jnp.sum(sums_ref[...], axis=0, keepdims=True)
    lane = lax.broadcasted_iota(jnp.int32, (1, 128), 1)
    total = jnp.sum(jnp.where(lane < 64, total, 0.0), axis=1, keepdims=True)
    return 1.0 / jnp.sqrt(total / NUMEL + 1e-06)


def fold_lanes(x):
    total = x[:, :128]
    for at in range(128, x.shape[1], 128):
        total = total + x[:, at : at + 128]
    return jnp.sum(total, axis=0, keepdims=True)


def pack_kernel(grad, master, moment, second, own, swap, part):
    core = lax.axis_index("gy_2")
    total = jnp.zeros((8, COLS), f32)
    for chip in range(8):
        for out, which in ((own, core), (swap, 1 - core)):
            rows = grad[2 * chip + which]
            out[chip, :, :COLS] = rows
            wide = rows.astype(f32)
            total = total + jnp.sum((wide * wide).reshape(ROWS // 8, 8, COLS), axis=0)
            cols = pl.ds(pl.multiple_of((2 * chip + which) * ACOLS, ACOLS), ACOLS)
            for n, state in enumerate((master, moment)):
                high, low = halves(state[:, cols])
                at = COLS + n * ACOLS
                out[chip, :AROWS, at : at + ACOLS] = high
                out[chip, AROWS:, at : at + ACOLS] = low
            coded = code_second(second[:, cols])
            out[chip, :AROWS, COLS + 2 * ACOLS :] = coded[:, :128]
            out[chip, AROWS:, COLS + 2 * ACOLS :] = coded[:, 128:]
    part[...] = fold_lanes(total)


def route_kernel(own, swapped, *outs):
    z, x, core = (lax.axis_index(axis) for axis in GY)
    for (dz, dx), out in zip(((0, 0),) + CHIP_STEPS, outs):
        chip = lax.rem(z + dz, 4) * 2 + lax.rem(x + dx, 2)
        out[core] = own[chip]
        out[1 - core] = swapped[chip]


def sum_kernel(arrived, part, summed, copies):
    total = arrived[0].astype(f32)
    for replica in range(1, 8):
        total = total + arrived[replica].astype(f32)
    summed[...] = total
    squared = jnp.sum((total * total).reshape(32, 8, ACOLS), axis=0)
    lane = lax.broadcasted_iota(jnp.int32, (1, 128), 1)
    row = part[...] + fold_lanes(squared)
    row = row + pltpu.roll(row, 64, 1)
    for group in range(16):
        top = largest(total[group * AROWS : (group + 1) * AROWS, :])
        row = jnp.where(lane == 64 + group, top, row)
    copies[...] = jnp.broadcast_to(row, (128, 128))


def sources():
    z, x = (lax.axis_index(axis) for axis in GY[:2])
    return [
        lax.rem(z + 4 - dz, 4) * 2 + lax.rem(x + dx, 2) for dz, dx in ((0, 0),) + CHIP_STEPS
    ]


def wide_cols(chip):
    return pl.ds(pl.multiple_of(chip * 2 * COLS, 2 * COLS), 2 * COLS)


def lanes(at):
    return slice(at * 128, (at + 1) * 128)


def expert_weight_kernel(sums, attn, *refs):
    blocks, early, streams, out = refs[:8], refs[8], refs[9:12], refs[12]
    held, weights, sems, out_sems = refs[13:]
    loads = []
    for n, chip in enumerate(sources()):
        loads.append(
            [
                pltpu.make_async_copy(array.at[:, wide_cols(chip)], held.at[m, n - EARLY], sems.at[n - EARLY, m])
                for m, array in enumerate(streams)
                if n >= EARLY
            ]
        )
        for copy in loads[n]:
            copy.start()
    clip = clip_of(sums)
    stores = []
    for n, (chip, block) in enumerate(zip(sources(), blocks)):
        for core in range(2):
            rows = pl.ds(pl.multiple_of((chip * 2 + core) * AROWS, AROWS), AROWS)
            summed = attn[rows, :]
            scaled = code(summed, largest(summed))
            weights[n, core, :AROWS, COLS:] = scaled[:, :128]
            weights[n, core, AROWS:, COLS:] = scaled[:, 128:]
        for copy in loads[n]:
            copy.wait()
        state = early.at[:, n] if n < EARLY else held.at[:, n - EARLY]
        for at in range(14):
            core, col = divmod(at, 7)
            new = adam_weight(
                block[core, :, lanes(col)].astype(f32),
                state[0, :, lanes(at)],
                state[1, :, lanes(at)],
                state[2, :, lanes(at)],
                clip,
            )
            weights[n, core, :, lanes(col)] = new.astype(bf16)
        store = pltpu.make_async_copy(weights.at[n], out.at[pl.ds(chip * 2, 2)], out_sems.at[n])
        store.start()
        stores.append(store)
    for store in stores:
        store.wait()


def expert_state_kernel(sums, *refs):
    blocks, state, outs = refs[:8], refs[8:11], refs[11:14]
    held, grads, news, sems, out_sems = refs[14:]
    loads = []
    for n, (chip, block) in enumerate(zip(sources(), blocks)):
        copies = [pltpu.make_async_copy(block.at[:, :, :COLS], grads.at[n], sems.at[n, 3])]
        for m, array in enumerate(state):
            copies.append(
                pltpu.make_async_copy(array.at[:, wide_cols(chip)], held.at[m, n], sems.at[n, m])
            )
        for copy in copies:
            copy.start()
        loads.append(copies)
    clip = clip_of(sums)
    stores = []
    for n, chip in enumerate(sources()):
        for copy in loads[n]:
            copy.wait()
        for at in range(14):
            core, col = divmod(at, 7)
            results = adam_update(
                grads[n, core, :, lanes(col)].astype(f32),
                held[0, n, :, lanes(at)],
                held[1, n, :, lanes(at)],
                held[2, n, :, lanes(at)],
                clip,
            )
            for m, result in enumerate(results):
                news[m, n, :, lanes(at)] = result
        for m, out in enumerate(outs):
            store = pltpu.make_async_copy(
                news.at[m, n], out.at[:, wide_cols(chip)], out_sems.at[n, m]
            )
            store.start()
            stores.append(store)
    for store in stores:
        store.wait()


def attn_weight_kernel(sums, attn, *refs):
    blocks, state, out, early, sems = refs[:8], refs[8:11], refs[11], refs[12], refs[13]
    loads = []
    for n, chip in enumerate(sources()[:EARLY]):
        for m, array in enumerate(state):
            loads.append(
                pltpu.make_async_copy(array.at[:, wide_cols(chip)], early.at[m, n], sems.at[n, m])
            )
            loads[-1].start()
    clip = clip_of(sums)
    for chip, block in zip(sources(), blocks):
        for core in range(2):
            rows = pl.ds(pl.multiple_of((chip * 2 + core) * AROWS, AROWS), AROWS)
            pair = COLS + 2 * ACOLS
            came = block[core, :AROWS, COLS:pair].astype(f32) + block[core, AROWS:, COLS:pair].astype(f32)
            for half in range(2):
                cols = lanes(half)
                new = adam_weight(
                    attn[rows, cols],
                    came[:, cols],
                    came[:, lanes(2 + half)],
                    decode_second(block[core, half * AROWS : (half + 1) * AROWS, pair:]),
                    clip,
                )
                out[rows, cols] = new.astype(bf16)
    for copy in loads:
        copy.wait()


def join_kernel(*refs):
    out, sems = refs[8], refs[9]
    x, y = (lax.axis_index(axis) for axis in GX)
    stores = []
    for half, row in enumerate((x, 1 - x)):
        for n, dy in enumerate((0,) + REPLICA_STEPS):
            slot = row * 4 + lax.rem(y + 4 - dy, 4)
            at = 4 * half + n
            stores.append(pltpu.make_async_copy(refs[at], out.at[slot], sems.at[at]))
            stores[-1].start()
    for store in stores:
        store.wait()


def finish_kernel(sums, arrived, *refs):
    state, weight, outs, news, sem, out_sems = refs[:3], refs[3], refs[4:7], refs[7], refs[8], refs[9]
    stores = [pltpu.make_async_copy(arrived.at[:, :, :COLS], weight, sem)]
    stores[0].start()
    clip = clip_of(sums)
    replica = lax.axis_index("gx_0") * 4 + lax.axis_index("gx_1")
    me = lax.axis_index("gy_0") * 4 + lax.axis_index("gy_1") * 2 + lax.axis_index("gy_2")
    mine = lax.broadcasted_iota(jnp.int32, (16, 128), 1) == 64 + me
    tops = sums[pl.ds(pl.multiple_of(replica * 16, 16), 16), :]
    tops = clip * jnp.sum(jnp.where(mine, tops, 0.0), axis=1, keepdims=True)
    for part in range(4):
        for group in range(4 * part, 4 * part + 4):
            for half in range(2):
                scaled = decode(
                    arrived[group, half * AROWS : (half + 1) * AROWS, COLS:], tops[group : group + 1, :]
                )
                cols = lanes(2 * group + half)
                results = adam_update(
                    scaled, state[0][:, cols], state[1][:, cols], state[2][:, cols], 1.0
                )
                for m, result in enumerate(results):
                    news[m, :, cols] = result
        cols = pl.ds(part * 4 * ACOLS, 4 * ACOLS)
        for m, out in enumerate(outs):
            store = pltpu.make_async_copy(
                news.at[m, :, cols], out.at[:, cols], out_sems.at[part, m]
            )
            store.start()
            stores.append(store)
    for store in stores:
        store.wait()


def chip_pairs(dz, dx):
    return [(z * 2 + x, (z + dz) % 4 * 2 + (x + dx) % 2) for z in range(4) for x in range(2)]


def local(
    expert_grad,
    attn_grad,
    expert_master,
    expert_moment,
    expert_second,
    attn_master,
    attn_moment,
    attn_second,
):
    arrived = lax.all_to_all(
        attn_grad.reshape(8, 256, ACOLS), GX, split_axis=0, concat_axis=0, tiled=True
    )

    own, swap, part = call(
        pack_kernel,
        (shape((8, ROWS, WIDE), bf16), shape((8, ROWS, WIDE), bf16), shape((1, 128), f32)),
        4000000,
    )(expert_grad.reshape(16, ROWS, COLS), attn_master, attn_moment, attn_second)
    swapped = lax.ppermute(swap, "gy_2", [(0, 1), (1, 0)])
    routed = call(route_kernel, (shape((2, ROWS, WIDE), bf16),) * 8, 1000000)(own, swapped)
    blocks = [routed[0]]
    for n, step in enumerate(CHIP_STEPS):
        blocks.append(lax.ppermute(routed[n + 1], GY[:2], chip_pairs(*step)))

    attn_sum, partial = call(
        sum_kernel, (shape((256, ACOLS), f32), shape((128, 128), f32)), 2000000
    )(arrived, part)
    sums = lax.all_to_all(
        partial.reshape(128, 1, 128), GX_GY, split_axis=0, concat_axis=0, tiled=True
    ).reshape(128, 128)

    vmem = pl.BlockSpec(memory_space=pltpu.VMEM)
    hbm = pl.BlockSpec(memory_space=pltpu.HBM)
    state = far(expert_master, expert_moment, expert_second)
    attn_block, early = call(
        attn_weight_kernel,
        (pltpu.VMEM((256, ACOLS), bf16), pltpu.VMEM((3, EARLY, ROWS, 2 * COLS), f32)),
        2000000,
        in_specs=[vmem] * 10 + [hbm] * 3,
        out_specs=[vmem] * 2,
        scratch_shapes=[pltpu.SemaphoreType.DMA((EARLY, 3))],
    )(*near(sums, attn_sum, *blocks), *state)
    other = lax.ppermute(attn_block, "gx_0", [(0, 1), (1, 0)])
    weights = call(
        expert_weight_kernel,
        pltpu.HBM((16, ROWS, BACK), bf16),
        8000000,
        in_specs=[vmem] * 11 + [hbm] * 3,
        out_specs=hbm,
        scratch_shapes=[
            pltpu.VMEM((3, 8 - EARLY, ROWS, 2 * COLS), f32),
            pltpu.VMEM((8, 2, ROWS, BACK), bf16),
            pltpu.SemaphoreType.DMA((8 - EARLY, 3)),
            pltpu.SemaphoreType.DMA((8,)),
        ],
    )(*near(sums, attn_sum, *blocks, early), *state)
    returned = lax.all_to_all(weights, GY, split_axis=0, concat_axis=0, tiled=True)
    pieces = []
    for block in (attn_block, other):
        pieces.append(block)
        for dy in REPLICA_STEPS:
            pieces.append(
                lax.ppermute(block, "gx_1", [(y, (y + dy) % 4) for y in range(4)])
            )
    e_master, e_moment, e_second = call(
        expert_state_kernel,
        (pltpu.HBM((ROWS, 16 * COLS), f32),) * 3,
        8000000,
        mib=16,
        in_specs=[vmem] + [pl.BlockSpec(memory_space=pl.ANY)] * 8 + [hbm] * 3,
        out_specs=[hbm] * 3,
        scratch_shapes=[
            pltpu.VMEM((3, 8, ROWS, 2 * COLS), f32),
            pltpu.VMEM((8, 2, ROWS, COLS), bf16),
            pltpu.VMEM((3, 8, ROWS, 2 * COLS), f32),
            pltpu.SemaphoreType.DMA((8, 4)),
            pltpu.SemaphoreType.DMA((8, 3)),
        ],
    )(sums, *blocks, *state)
    attn_weight = call(
        join_kernel,
        pltpu.HBM((8, 256, ACOLS), bf16),
        1000000,
        in_specs=[vmem] * 8,
        out_specs=hbm,
        scratch_shapes=[pltpu.SemaphoreType.DMA((8,))],
    )(*near(*pieces))
    expert_weight, a_master, a_moment, a_second = call(
        finish_kernel,
        (pltpu.HBM((16, ROWS, COLS), bf16),) + (pltpu.HBM((AROWS, 16 * ACOLS), f32),) * 3,
        2000000,
        in_specs=[vmem] * 5,
        out_specs=[hbm] * 4,
        scratch_shapes=[
            pltpu.VMEM((3, AROWS, 16 * ACOLS), f32),
            pltpu.SemaphoreType.DMA,
            pltpu.SemaphoreType.DMA((4, 3)),
        ],
    )(*near(sums, returned), attn_master, attn_moment, attn_second)
    return (
        e_master,
        e_moment,
        e_second,
        a_master,
        a_moment,
        a_second,
        expert_weight.reshape(1, 16 * ROWS, COLS),
        attn_weight.reshape(2048, ACOLS),
    )


def solution(mesh):
    split = Mesh(mesh.devices.reshape(2, 4, 4, 2, 2), GX_GY)
    placed = (P(GX, None, GY),) * 2 + (P(GX_GY, None),) * 6

    return jax.shard_map(
        local,
        mesh=split,
        in_specs=placed,
        out_specs=(P(GX_GY, None),) * 6 + (P(GX, None, GY), P(None, GY)),
        check_vma=False,
    )
```
